256 devices in a mesh: lat: 8 (over x, z_hi), lon: 32 (over y, z_lo, core).
Axes of the slice: x: 4, y: 4, z: 8 (z_hi: 2, z_lo: 4; z = z_hi * 4 + z_lo), core: 2. Of those that a mesh axis runs over, the one named last changes fastest.
Arguments:
- tracers: float32 [100, 2, 128, 4096], P(None, None, 'lat', 'lon'), may hold values from 0.1 to 30, as said below
- offsets: int32 [2, 2, 128, 4096], P(None, None, 'lat', 'lon'), may hold values from -3 to 2
- target: float32 [100, 2, 128], P(None, None, 'lat'), may hold values from 0.3 to 4
- band_mask: int32 [128], P('lat'), may hold values 0 or 1
Outputs:
- nudged: float32 [100, 2, 128, 4096], P(None, None, 'lat', 'lon')
The draws below stay inside these ranges and needn't reach their ends.
Inputs may be any that keep to these rules, and one draw needn't show every extreme that they name: Each cell's offsets are drawn independently of its neighbours', in both directions. `tracers`: positive mixing ratios.
All inputs are finite; a program needn't handle non-finite values. No bound on the sum of `band_mask` on one device may be relied on, other than what follows from the above.
Results may differ from the reference program's by a relative error of at most 0.00002.
Values sent between devices are 32-bit elements; how exact they have to be, the bound alone decides.
A program may use at most 64 MiB of HBM per device.

```python
import math
import jax
import jax.numpy as jnp
from jax import lax

TRACERS = 100
LEV = 2
NLAT = 128
NLON = 4096


def draw_tracers(key, part):
    first_key = jax.random.fold_in(jax.random.fold_in(key, 17), 0)
    shape = (TRACERS, LEV, NLAT, NLON)
    position = jnp.arange(NLON, dtype=jnp.float32) / NLON
    base = jnp.exp(jax.random.uniform(first_key, shape, jnp.float32, math.log(0.2), math.log(2.0)))
    return base * (1.0 + 2.0 * position)


def with_ends(result, stream_key, low, top_value):
    place = [jax.random.randint(jax.random.fold_in(stream_key, axis), (), 0, length) for axis, length in enumerate(result.shape)]
    main_axis = result.shape.index(max(result.shape))
    next_to = place[:main_axis] + [(place[main_axis] + 1) % result.shape[main_axis]] + place[main_axis + 1:]
    return result.at[tuple(place)].set(low).at[tuple(next_to)].set(top_value)


def block_scale(key, shape, pieces, low, high):
    gain, own = 1.0, jax.random.fold_in(key, 6)
    for dim, shards_of in pieces:
        steps = jnp.exp(jax.random.uniform(jax.random.fold_in(own, dim), (shards_of,), jnp.float32, low / len(pieces), high / len(pieces)))
        gain = gain * jnp.repeat(steps, shape[dim] // shards_of).reshape([-1 if axis == dim else 1 for axis in range(len(shape))])
    return gain


def setup_inputs(seed: int = 0) -> dict:
    keys = jax.random.split(jax.random.key(seed), 5)
    return {
        "tracers": draw_tracers(jax.random.fold_in(keys[4], 71), 0),
        "offsets": with_ends(jax.random.randint(keys[1], (2, LEV, NLAT, NLON), -3, 3), jax.random.fold_in(keys[1], 1), -3, 2).astype(jnp.int32),
        "target": jnp.clip(jnp.exp(math.log(4.0) - 2.5902671 * jax.random.uniform(keys[2], (TRACERS, LEV, NLAT), jnp.float32) ** block_scale(keys[2], (TRACERS, LEV, NLAT), ((2, 8),), -0.2, 0.2)), 0.3, 4.0),
        "band_mask": with_ends((jax.random.randint(keys[3], (NLAT,), 0, 2) < 1).astype(jnp.int32), jax.random.fold_in(keys[3], 1), 0, 1),
    }


LON_TAPS = (-0.0546875, 0.8203125, 0.2734375, -0.0390625)
LAT_TAPS = (-0.0625, 0.5625, 0.5625, -0.0625)

def reach_weights(offset, taps):
    weights = [jnp.zeros(offset.shape, jnp.float32) for index in range(9)]
    for shift in range(-3, 3):
        matches = (offset == shift).astype(jnp.float32)
        for tap in range(4):
            where_to = shift + tap - 1 + 4
            weights[where_to] = weights[where_to] + taps[tap] * matches
    return weights

def stencil(padded, lon_weights, lat_weights, rows, cols):
    total_sum = jnp.zeros(padded.shape[:-2] + (rows, cols), jnp.float32)
    for row_shift in range(9):
        row_part = padded[..., row_shift:row_shift + rows, :]
        inner = jnp.zeros_like(total_sum)
        for col_shift in range(9):
            inner = inner + lon_weights[col_shift] * row_part[..., col_shift:col_shift + cols]
        total_sum = total_sum + lat_weights[row_shift] * inner
    return total_sum

def reference(tracers, offsets, target, band_mask):
    rows = tracers.shape[2]
    cols = tracers.shape[3]
    lon_weights = reach_weights(offsets[0], LON_TAPS)
    lat_weights = reach_weights(offsets[1], LAT_TAPS)
    mask_rows = band_mask.astype(jnp.float32)

    def one_tracer(inputs):
        field, goal = inputs
        wrapped = jnp.concatenate([field[..., -4:], field, field[..., :4]], axis=-1)
        padded = jnp.pad(wrapped, ((0, 0), (4, 4), (0, 0)))
        advected = stencil(padded, lon_weights, lat_weights, rows, cols)
        rms = jnp.sqrt(lax.optimization_barrier(jnp.mean(advected * advected, axis=-1)) + 1e-06)
        factor = 1.0 + 0.5 * mask_rows[None, :] * (goal / rms - 1.0)
        return advected * factor[..., None]
    return lax.map(one_tracer, (tracers, target))
```

```python
import functools

import jax
import jax.numpy as jnp
from jax import lax
from jax.experimental import pallas as pl
from jax.experimental.pallas import tpu as pltpu
from jax.sharding import PartitionSpec as P

LON_TAPS = (-0.0546875, 0.8203125, 0.2734375, -0.0390625)
LAT_TAPS = (-0.0625, 0.5625, 0.5625, -0.0625)
MESH = pl.DeviceIdType.MESH
F32 = jnp.float32
BF16 = jnp.bfloat16
TP = 112
KW = 384
BANDS = 24
ZGROUP = 4
CORES = 2


def tap_select(distance, taps):
    out = jnp.zeros(distance.shape, F32)
    for k in range(4):
        out = jnp.where(distance == k - 1, taps[k], out)
    return out


def lon_matrix(o0, lcat):
    rows = lax.broadcasted_iota(jnp.int32, (128, 128), 0)
    lanes = lax.broadcasted_iota(jnp.int32, (128, 128), 1)
    main = tap_select(rows - lanes - o0, LON_TAPS).astype(BF16)
    lcat[0:128, :] = main
    lcat[128:256, :] = main
    e = lax.broadcasted_iota(jnp.int32, (16, 128), 0) % 8
    lanes = lax.broadcasted_iota(jnp.int32, (16, 128), 1)
    edge = jnp.where(e < 4, e - 4, e + 124)
    lcat[256:272, :] = tap_select(edge - lanes - o0, LON_TAPS).astype(BF16)


def kernel(nt, nlat, nlon, x_hbm, off_hbm, target_ref, mask_ref, out_ref,
           xv, xb, offv, es, er, ob, zs, zr, acc, lcat, sums, sums_t, ra, rb,
           local_sem, e_send, e_recv, o_send, o_recv, z_send, z_recv, a_send, a_recv, b_send, b_recv):
    lat = lax.axis_index("lat")
    lon = lax.axis_index("lon")
    left = lax.rem(lon + nlon - 1, nlon)
    right = lax.rem(lon + 1, nlon)
    core = lax.rem(lon, CORES)
    zlo = lax.rem(lon // CORES, ZGROUP)
    ny = nlon // (ZGROUP * CORES)
    yy = lon // (ZGROUP * CORES)

    load_x = pltpu.make_async_copy(x_hbm, xv.at[pl.ds(0, nt * 32)], local_sem.at[0])
    load_x.start()
    load_off = pltpu.make_async_copy(off_hbm, offv, local_sem.at[1])
    load_off.start()

    def z_peer(k):
        return {"lon": (yy * ZGROUP + lax.rem(zlo + k, ZGROUP)) * CORES + core}

    def y_peer(k):
        me = yy * CORES + core
        other = lax.rem(me + k, ny * CORES)
        return {"lon": ((other // CORES) * ZGROUP + zlo) * CORES + lax.rem(other, CORES)}

    barrier = pltpu.get_barrier_semaphore()

    def greet(device):
        pl.semaphore_signal(barrier, inc=1, device_id=device, device_id_type=MESH)

    has_up = lat > 0
    has_down = lat < nlat - 1

    @pl.when(has_up)
    def _():
        greet({"lat": lat - 1})

    @pl.when(has_down)
    def _():
        greet({"lat": lat + 1})

    greet({"lon": left})
    greet({"lon": right})
    for k in range(1, ZGROUP):
        greet(z_peer(k))
    for k in range(1, ny * CORES):
        greet(y_peer(k))

    xv[pl.ds(nt * 32, (TP - nt) * 32), :] = jnp.zeros(((TP - nt) * 32, 128), F32)
    for l in range(2):
        for first in (0, 20):
            xb[pl.ds((l * BANDS + first) * TP, 4 * TP), :] = jnp.zeros((4 * TP, KW), BF16)
    lcat[272:384, :] = jnp.zeros((112, 128), BF16)
    lane = lax.broadcasted_iota(jnp.int32, (TP, 128), 1)

    load_off.wait()
    load_x.wait()

    def pack(lj, carry):
        to_left, to_right = carry
        v = xv[pl.ds(lj, TP, stride=32), :]
        rolled = pltpu.roll(v, 4 * lj, 1)
        group = lane // 4
        to_left = jnp.where(group == lj, rolled, to_left)
        to_right = jnp.where(group == lax.rem(lj + 31, 32), rolled, to_right)
        hi = v.astype(BF16)
        lo = (v - hi.astype(F32)).astype(BF16)
        row = pl.multiple_of(((lj // 16) * BANDS + 4 + lax.rem(lj, 16)) * TP, 16)
        xb[pl.ds(row, TP), 0:128] = hi
        xb[pl.ds(row, TP), 128:256] = lo
        return to_left, to_right

    zero = jnp.zeros((TP, 128), F32)
    to_left, to_right = lax.fori_loop(0, 32, pack, (zero, zero))
    es[0] = to_left
    es[1] = to_right

    pl.semaphore_wait(
        barrier, has_up.astype(jnp.int32) + has_down.astype(jnp.int32) + 2 + (ZGROUP - 1) + (ny * CORES - 1)
    )

    def o_copy(direction):
        return pltpu.make_async_remote_copy(
            src_ref=offv.reshape(2, 2, 16, 128).at[:, :, pl.ds(12 * direction, 4), :],
            dst_ref=ob.at[direction],
            send_sem=o_send.at[direction], recv_sem=o_recv.at[direction],
            device_id={"lat": lat - 1 + 2 * direction}, device_id_type=MESH)

    def e_copy(side):
        return pltpu.make_async_remote_copy(
            src_ref=es.at[side], dst_ref=er.at[1 - side],
            send_sem=e_send.at[side], recv_sem=e_recv.at[1 - side],
            device_id={"lon": left if side == 0 else right}, device_id_type=MESH)

    def z_copy(direction, s):
        return pltpu.make_async_remote_copy(
            src_ref=zs.at[direction, s, pl.ds(0, nt)], dst_ref=zr.at[direction, s, pl.ds(0, nt)],
            send_sem=z_send.at[direction, s], recv_sem=z_recv.at[direction, s],
            device_id={"lat": lat + 1 - 2 * direction}, device_id_type=MESH)

    @pl.when(has_up)
    def _():
        o_copy(0).start()

    @pl.when(has_down)
    def _():
        o_copy(1).start()

    e_copy(0).start()
    e_copy(1).start()
    for side in range(2):
        pltpu.make_async_remote_copy(
            src_ref=es.at[side], dst_ref=er.at[side], send_sem=e_send.at[side], recv_sem=e_recv.at[side],
            device_id={"lon": left}, device_id_type=MESH).wait_recv()

    def edges(lj, _):
        shift = lax.rem(132 - 4 * lj, 128)
        a = pltpu.roll(er[0], shift, 1)
        b = pltpu.roll(er[1], shift, 1)
        e = jnp.where(lane < 4, a, b)
        hi = e.astype(BF16).astype(F32)
        both = jnp.where(lane < 8, hi, pltpu.roll(e - hi, 8, 1))
        row = pl.multiple_of(((lj // 16) * BANDS + 4 + lax.rem(lj, 16)) * TP, 16)
        xb[pl.ds(row, TP), 256:384] = both.astype(BF16)
        return 0

    lax.fori_loop(0, 32, edges, 0)

    for direction in range(2):
        exists = has_down if direction == 0 else has_up

        @pl.when(exists)
        def _():
            pltpu.make_async_remote_copy(
                src_ref=ob.at[direction], dst_ref=ob.at[direction],
                send_sem=o_send.at[direction], recv_sem=o_recv.at[direction],
                device_id={"lat": lat + 1 - 2 * direction}, device_id_type=MESH).wait_recv()

            def part(s, _):
                l, jj = s // 4, lax.rem(s, 4)
                o0 = ob[direction, 0, l, pl.ds(jj, 1), :]
                o1 = ob[direction, 1, l, pl.ds(jj, 1), :]
                lon_matrix(o0, lcat)
                start = pl.multiple_of((l * BANDS + 4 + 12 * (1 - direction)) * TP, 16)
                y = jnp.dot(xb[pl.ds(start, 4 * TP), :], lcat[...], preferred_element_type=F32)
                total = jnp.zeros((TP, 128), F32)
                for hh in range(4):
                    w = tap_select(hh + (4 if direction else -4) - jj - o1, LAT_TAPS)
                    total = total + w * y[hh * TP:(hh + 1) * TP]
                zs[direction, s] = total
                z_copy(direction, s).start()
                return 0

            lax.fori_loop(0, 8, part, 0)

    def own(lj, _):
        l, j = lj // 16, lax.rem(lj, 16)
        o0 = offv[pl.ds(lj, 1), :]
        o1 = offv[pl.ds(32 + lj, 1), :]
        lon_matrix(o0, lcat)
        start = pl.multiple_of((l * BANDS + j) * TP, 16)
        y = jnp.dot(xb[pl.ds(start, 9 * TP), :], lcat[...], preferred_element_type=F32)
        total = jnp.zeros((TP, 128), F32)
        for rr in range(9):
            w = tap_select(rr - 4 - o1, LAT_TAPS)
            total = total + w * y[rr * TP:(rr + 1) * TP]
        acc[lj] = total
        return 0

    lax.fori_loop(0, 32, own, 0)

    for direction in range(2):
        exists = has_up if direction == 0 else has_down

        @pl.when(exists)
        def _():
            def add(s, _):
                z_copy(direction, s).wait_recv()
                lj = (s // 4) * 16 + 12 * direction + lax.rem(s, 4)
                acc[lj] = acc[lj] + zr[direction, s]
                return 0

            lax.fori_loop(0, 8, add, 0)

    def square(lj, total):
        a = acc[lj]
        return jnp.where(lane == lj, jnp.sum(a * a, axis=1, keepdims=True), total)

    sums[0:TP, :] = lax.fori_loop(0, 32, square, zero)
    sums[TP:128, :] = jnp.zeros((128 - TP, 128), F32)
    sums_t[...] = jnp.transpose(sums[...])[0:32]

    def exchange(peer, group, me, slots, send, recv, src):
        copies = []
        for k in range(1, group):
            copies.append(pltpu.make_async_remote_copy(
                src_ref=src, dst_ref=slots.at[k], send_sem=send.at[k], recv_sem=recv.at[k],
                device_id=peer(k), device_id_type=MESH))
        for c in copies:
            c.start()
        total = src[...]
        for k, c in enumerate(copies):
            c.wait_recv()
            total = total + slots[k + 1]
        return total, copies

    total, a_copies = exchange(z_peer, ZGROUP, zlo, ra, a_send, a_recv, sums_t)
    ra[0] = total
    total, b_copies = exchange(y_peer, ny * CORES, 0, rb, b_send, b_recv, ra.at[0])

    rms = jnp.sqrt(total * (1.0 / (128 * nlon)) + 1e-06)
    row = lax.rem(lax.broadcasted_iota(jnp.int32, (32, 128), 0), 16)
    mask = jnp.zeros((32, 128), F32)
    for j in range(16):
        mask = jnp.where(row == j, mask_ref[j].astype(F32), mask)
    factor = 1.0 + 0.5 * mask * (target_ref[...] / rms - 1.0)
    sums[0:32, :] = factor
    factor_t = jnp.transpose(sums[...])[0:TP]

    def scale(lj, _):
        column = jnp.sum(jnp.where(lane == lj, factor_t, 0.0), axis=1, keepdims=True)
        out_ref[pl.ds(lj, nt, stride=32), :] = (acc[lj] * column)[0:nt]
        return 0

    lax.fori_loop(0, 32, scale, 0)

    e_copy(0).wait_send()
    e_copy(1).wait_send()
    for c in a_copies + b_copies:
        c.wait_send()
    for direction in range(2):
        exists = has_down if direction == 0 else has_up

        @pl.when(exists)
        def _():
            o_copy(1 - direction).wait_send()
            lax.fori_loop(0, 8, lambda s, _: (z_copy(direction, s).wait_send(), 0)[1], 0)


def solution(mesh):
    nlat, nlon = mesh.shape["lat"], mesh.shape["lon"]

    def body(tracers, offsets, target, band_mask):
        nt = tracers.shape[0]
        nb = nlon // ZGROUP
        target_t = jnp.pad(jnp.transpose(target, (1, 2, 0)).reshape(32, nt), ((0, 0), (0, 128 - nt)), constant_values=1.0)
        vmem = pltpu.VMEM
        out = pl.pallas_call(
            functools.partial(kernel, nt, nlat, nlon),
            out_shape=jax.ShapeDtypeStruct((nt * 32, 128), F32),
            in_specs=[
                pl.BlockSpec(memory_space=pl.ANY),
                pl.BlockSpec(memory_space=pl.ANY),
                pl.BlockSpec(memory_space=pltpu.VMEM),
                pl.BlockSpec(memory_space=pltpu.SMEM),
            ],
            out_specs=pl.BlockSpec(memory_space=pltpu.VMEM),
            scratch_shapes=[
                vmem((TP * 32, 128), F32),
                vmem((2 * BANDS * TP, KW), BF16),
                vmem((64, 128), jnp.int32),
                vmem((2, TP, 128), F32),
                vmem((2, TP, 128), F32),
                vmem((2, 2, 2, 4, 128), jnp.int32),
                vmem((2, 8, TP, 128), F32),
                vmem((2, 8, TP, 128), F32),
                vmem((32, TP, 128), F32),
                vmem((KW, 128), BF16),
                vmem((128, 128), F32),
                vmem((32, 128), F32),
                vmem((ZGROUP, 32, 128), F32),
                vmem((nb, 32, 128), F32),
                pltpu.SemaphoreType.DMA((2,)),
                pltpu.SemaphoreType.DMA((2,)),
                pltpu.SemaphoreType.DMA((2,)),
                pltpu.SemaphoreType.DMA((2,)),
                pltpu.SemaphoreType.DMA((2,)),
                pltpu.SemaphoreType.DMA((2, 8)),
                pltpu.SemaphoreType.DMA((2, 8)),
                pltpu.SemaphoreType.DMA((ZGROUP,)),
                pltpu.SemaphoreType.DMA((ZGROUP,)),
                pltpu.SemaphoreType.DMA((nb,)),
                pltpu.SemaphoreType.DMA((nb,)),
            ],
            compiler_params=pltpu.CompilerParams(
                collective_id=0, has_side_effects=True, vmem_limit_bytes=48 * 1024 * 1024
            ),
        )(tracers.reshape(nt * 32, 128), offsets.reshape(64, 128), target_t, band_mask)
        return out.reshape(tracers.shape)

    placed = (
        P(None, None, "lat", "lon"),
        P(None, None, "lat", "lon"),
        P(None, None, "lat"),
        P("lat"),
    )
    return jax.shard_map(
        body, mesh=mesh, in_specs=placed, out_specs=P(None, None, "lat", "lon"), check_vma=False
    )
```

```python
import functools

import jax
import jax.numpy as jnp
from jax import lax
from jax.experimental import pallas as pl
from jax.experimental.pallas import tpu as pltpu
from jax.sharding import PartitionSpec as P

LON_TAPS = (-0.0546875, 0.8203125, 0.2734375, -0.0390625)
LAT_TAPS = (-0.0625, 0.5625, 0.5625, -0.0625)
MESH = pl.DeviceIdType.MESH
F32 = jnp.float32
BF16 = jnp.bfloat16
TP = 112
KW = 384
BANDS = 24
ZGROUP = 4
CORES = 2
PITCH = 40
STEP = 4
CAP = 512
FLAG = 120


def tap_select(distance, taps):
    out = jnp.zeros(distance.shape, F32)
    for k in range(4):
        out = jnp.where(distance == k - 1, taps[k], out)
    return out


def lon_matrix(column, lcat, base):
    rows = lax.broadcasted_iota(jnp.int32, (128, 128), 0)
    main = tap_select(rows - column, LON_TAPS).astype(BF16)
    lcat[base:base + 128, :] = main
    lcat[base + 128:base + 256, :] = main
    e = lax.broadcasted_iota(jnp.int32, (16, 128), 0) % 8
    edge = jnp.where(e < 4, e - 4, e + 124)
    lcat[base + 256:base + 272, :] = tap_select(edge - column, LON_TAPS).astype(BF16)


def places(o1, direction):
    row = lax.broadcasted_iota(jnp.int32, (8, 128), 0)
    reach = lax.rem(row, 4) + o1
    need = reach >= 2 if direction else reach <= 0
    m = jnp.where(need, 1.0, 0.0)
    i = lax.broadcasted_iota(jnp.int32, (128, 128), 0)
    k = lax.broadcasted_iota(jnp.int32, (128, 128), 1)
    earlier = jnp.where(i < k, 1.0, 0.0).astype(BF16)
    m16 = jnp.concatenate([m, m], axis=0).astype(BF16)
    before = jnp.dot(m16, earlier, preferred_element_type=F32)[0:8]
    own = jnp.broadcast_to(jnp.sum(m, axis=1, keepdims=True), (8, 128))
    count = own
    for n in range(1, 8):
        above = jnp.where(row >= n, pltpu.roll(own, n, 0), 0.0)
        before = before + above
        count = count + above
    return jnp.where(need, before, -1.0).astype(jnp.int32), count


def kernel(dense, nt, nlat, nlon, x_hbm, off_hbm, target_hbm, mask_hbm, out_ref, flag_ref,
           xv, xb, offv, target_v, mask_v, es, er, ob, zs, zr, acc, lcat, sums, sums_t, ra, rb,
           pick, spread, fs, fr,
           local_sem, e_send, e_recv, o_send, o_recv, z_send, z_recv, a_send, a_recv, b_send, b_recv,
           f_send, f_recv):
    lat = lax.axis_index("lat")
    lon = lax.axis_index("lon")
    left = lax.rem(lon + nlon - 1, nlon)
    right = lax.rem(lon + 1, nlon)
    core = lax.rem(lon, CORES)
    zlo = lax.rem(lon // CORES, ZGROUP)
    ny = nlon // (ZGROUP * CORES)
    yy = lon // (ZGROUP * CORES)
    chunks = 8 if dense else CAP // 128

    load_x = pltpu.make_async_copy(
        x_hbm, xv.reshape(TP, PITCH, 128).at[pl.ds(0, nt), pl.ds(0, 32), :], local_sem.at[0])
    load_x.start()
    load_off = pltpu.make_async_copy(off_hbm, offv, local_sem.at[1])
    load_off.start()
    load_target = pltpu.make_async_copy(target_hbm, target_v, local_sem.at[2])
    load_target.start()
    load_mask = pltpu.make_async_copy(mask_hbm, mask_v, local_sem.at[3])
    load_mask.start()

    def z_peer(k):
        return {"lon": (yy * ZGROUP + lax.rem(zlo + k, ZGROUP)) * CORES + core}

    def y_peer(k):
        me = yy * CORES + core
        other = lax.rem(me + k, ny * CORES)
        return {"lon": ((other // CORES) * ZGROUP + zlo) * CORES + lax.rem(other, CORES)}

    def lat_peer(k):
        return {"lat": lax.rem(lat + k, nlat)}

    barrier = pltpu.get_barrier_semaphore()

    def greet(device):
        pl.semaphore_signal(barrier, inc=1, device_id=device, device_id_type=MESH)

    has_up = lat > 0
    has_down = lat < nlat - 1
    for k in range(1, nlat):
        greet(lat_peer(k))
    greet({"lon": left})
    greet({"lon": right})
    for k in range(1, ZGROUP):
        greet(z_peer(k))
    for k in range(1, ny * CORES):
        greet(y_peer(k))

    xv[pl.ds(nt * PITCH, (TP - nt) * PITCH), :] = jnp.zeros(((TP - nt) * PITCH, 128), F32)
    for l in range(2):
        for first in (0, 20):
            xb[pl.ds((l * BANDS + first) * TP, 4 * TP), :] = jnp.zeros((4 * TP, KW), BF16)
        lcat[l * KW + 272:(l + 1) * KW, :] = jnp.zeros((112, 128), BF16)
    lane = lax.broadcasted_iota(jnp.int32, (TP, 128), 1)

    load_off.wait()
    load_target.wait()
    load_mask.wait()
    load_x.wait()
    row = lax.rem(lax.broadcasted_iota(jnp.int32, (32, 128), 0), 16)
    mask = jnp.zeros((32, 128), F32)
    for j in range(16):
        mask = jnp.where(row == j, mask_v[j].astype(F32) * 0.5, mask)
    mask = mask[:, 0:nt]

    group = lane // 4

    def pack(step, carry):
        to_left, to_right = carry
        for i in range(STEP):
            lj = step * STEP + i
            v = xv[pl.ds(lj, TP, stride=PITCH), :]
            rolled = pltpu.roll(v, 4 * lj, 1)
            to_left = jnp.where(group == lj, rolled, to_left)
            to_right = jnp.where(group == lax.rem(lj + 31, 32), rolled, to_right)
            hi = v.astype(BF16)
            lo = (v - hi.astype(F32)).astype(BF16)
            row = pl.multiple_of(((lj // 16) * BANDS + 4 + lax.rem(lj, 16)) * TP, 16)
            xb[pl.ds(row, TP), 0:128] = hi
            xb[pl.ds(row, TP), 128:256] = lo
        return to_left, to_right

    zero = jnp.zeros((TP, 128), F32)
    with jax.named_scope("pack"):
        to_left, to_right = lax.fori_loop(0, 32 // STEP, pack, (zero, zero))
    es[0] = to_left
    es[1] = to_right

    with jax.named_scope("barw"):
        pl.semaphore_wait(barrier, (nlat - 1) + 2 + (ZGROUP - 1) + (ny * CORES - 1))

    ob4 = ob.reshape(2, 2, 2, 4, 128)

    def o_copy(direction):
        return pltpu.make_async_remote_copy(
            src_ref=offv.reshape(2, 2, 16, 128).at[:, :, pl.ds(12 * direction, 4), :],
            dst_ref=ob4.at[direction],
            send_sem=o_send.at[direction], recv_sem=o_recv.at[direction],
            device_id={"lat": lat - 1 + 2 * direction}, device_id_type=MESH)

    def e_copy(side):
        return pltpu.make_async_remote_copy(
            src_ref=es.at[side], dst_ref=er.at[1 - side],
            send_sem=e_send.at[side], recv_sem=e_recv.at[1 - side],
            device_id={"lon": left if side == 0 else right}, device_id_type=MESH)

    def z_copy(direction, s):
        return pltpu.make_async_remote_copy(
            src_ref=zs.at[direction, s, pl.ds(0, nt)], dst_ref=zr.at[direction, s, pl.ds(0, nt)],
            send_sem=z_send.at[direction, s], recv_sem=z_recv.at[direction, s],
            device_id={"lat": lat + 1 - 2 * direction}, device_id_type=MESH)

    @pl.when(has_up)
    def _():
        o_copy(0).start()

    @pl.when(has_down)
    def _():
        o_copy(1).start()

    e_copy(0).start()
    e_copy(1).start()

    f_copies = []
    place = []
    if not dense:
        flag = jnp.zeros((8, 128), F32)
        for direction in range(2):
            o1 = jnp.concatenate(
                [offv[pl.ds(32 + 12 * direction, 4), :], offv[pl.ds(48 + 12 * direction, 4), :]], axis=0)
            p, count = places(o1, direction)
            place.append(p)
            exists = has_up if direction == 0 else has_down
            flag = jnp.maximum(flag, jnp.where(count > CAP, exists.astype(F32), 0.0))
        fs[...] = jnp.broadcast_to(jnp.max(flag, axis=(0, 1), keepdims=True), (1, 128))
        for k in range(1, nlat):
            f_copies.append(pltpu.make_async_remote_copy(
                src_ref=fs, dst_ref=fr.at[k], send_sem=f_send.at[k], recv_sem=f_recv.at[k],
                device_id=lat_peer(k), device_id_type=MESH))
        for c in f_copies:
            c.start()

    with jax.named_scope("ewait"):
        for side in range(2):
            pltpu.make_async_remote_copy(
                src_ref=es.at[side], dst_ref=er.at[side], send_sem=e_send.at[side], recv_sem=e_recv.at[side],
                device_id={"lon": left}, device_id_type=MESH).wait_recv()

    def edges(first, step):
        for i in range(STEP):
            lj = 16 * (step // 2) + first + (4 if first else 12) * lax.rem(step, 2) + i
            shift = lax.rem(132 - 4 * lj, 128)
            a = pltpu.roll(er[0], shift, 1)
            b = pltpu.roll(er[1], shift, 1)
            e = jnp.where(lane < 4, a, b)
            hi = e.astype(BF16).astype(F32)
            both = jnp.where(lane < 8, hi, pltpu.roll(e - hi, 8, 1))
            row = pl.multiple_of(((lj // 16) * BANDS + 4 + lax.rem(lj, 16)) * TP, 16)
            xb[pl.ds(row, TP), 256:384] = both.astype(BF16)
        return 0

    with jax.named_scope("edges"):
        lax.fori_loop(0, 4, lambda step, _: edges(0, step), 0)

    def send_dense(direction):
        def part(s, _):
            l, jj = s // 4, lax.rem(s, 4)
            o0 = ob[pl.ds(16 * direction + s, 1), :]
            o1 = ob[pl.ds(16 * direction + 8 + s, 1), :]
            lon_matrix(o0 + lane[0:1], lcat, 0)
            start = pl.multiple_of((l * BANDS + 4 + 12 * (1 - direction)) * TP, 16)
            y = jnp.dot(xb[pl.ds(start, 4 * TP), :], lcat[0:KW, :], preferred_element_type=F32)
            total = jnp.zeros((TP, 128), F32)
            for hh in range(4):
                w = tap_select(hh + (4 if direction else -4) - jj - o1, LAT_TAPS)
                total = total + w * y[hh * TP:(hh + 1) * TP]
            zs[direction, s] = total
            z_copy(direction, s).start()
            return 0

        lax.fori_loop(0, 8, part, 0)

    def send_packed(direction):
        o0 = ob[pl.ds(16 * direction, 8), :]
        o1 = ob[pl.ds(16 * direction + 8, 8), :]
        row = lax.broadcasted_iota(jnp.int32, (8, 128), 0)
        column = lax.broadcasted_iota(jnp.int32, (8, 128), 1) + o0
        reach = lax.rem(row, 4) + o1
        number, _ = places(o1, direction)
        number_t = jnp.transpose(jnp.concatenate([number, jnp.zeros((120, 128), jnp.int32)], axis=0))
        slot = lax.broadcasted_iota(jnp.int32, (128, CAP), 1)
        row16 = lax.broadcasted_iota(jnp.int32, (16, 128), 0)
        cells = []
        for s in range(8):
            pick[s * 128:(s + 1) * 128, :] = jnp.where(number_t[:, s:s + 1] == slot, 1.0, 0.0).astype(BF16)
            v = jnp.where(row16 == 0, column[s:s + 1], jnp.where(row16 == 1, reach[s:s + 1], s // 4))
            cells.append(v.astype(F32).astype(BF16))
        known = jnp.dot(jnp.concatenate(cells, axis=1), pick[...], preferred_element_type=F32).astype(jnp.int32)
        for c in range(CAP // 128):
            column = known[0:1, c * 128:(c + 1) * 128]
            reach = known[1:2, c * 128:(c + 1) * 128]
            level = known[2:3, c * 128:(c + 1) * 128]
            y = jnp.zeros((4 * TP, 128), F32)
            for l in range(2):
                lon_matrix(jnp.where(level == l, column, 4096), lcat, l * KW)
                start = (l * BANDS + 4 + 12 * (1 - direction)) * TP
                y = y + jnp.dot(xb[start:start + 4 * TP, :], lcat[l * KW:(l + 1) * KW, :], preferred_element_type=F32)
            total = jnp.zeros((TP, 128), F32)
            for hh in range(4):
                w = tap_select(hh + (4 if direction else -4) - reach, LAT_TAPS)
                total = total + w * y[hh * TP:(hh + 1) * TP]
            zs[direction, c] = total
            z_copy(direction, c).start()

    for direction in range(2):
        @pl.when(has_up if direction else has_down)
        def _():
            with jax.named_scope("owait"):
                pltpu.make_async_remote_copy(
                    src_ref=ob4.at[direction], dst_ref=ob4.at[direction],
                    send_sem=o_send.at[direction], recv_sem=o_recv.at[direction],
                    device_id={"lat": lat + 1 - 2 * direction}, device_id_type=MESH).wait_recv()
            with jax.named_scope("part"):
                if dense:
                    send_dense(direction)
                else:
                    send_packed(direction)

    if not dense:
        slot = lax.broadcasted_iota(jnp.int32, (CAP, 128), 0)
        with jax.named_scope("spread"):
            for direction in range(2):
                for s in range(8):
                    spread[direction, :, s * 128:(s + 1) * 128] = jnp.where(
                        place[direction][s:s + 1] == slot, 1.0, 0.0).astype(BF16)

    with jax.named_scope("edges2"):
        lax.fori_loop(0, 4, lambda step, _: edges(4, step), 0)

    def own(lj, _):
        l, j = lj // 16, lax.rem(lj, 16)
        o0 = offv[pl.ds(lj, 1), :]
        o1 = offv[pl.ds(32 + lj, 1), :]
        lon_matrix(o0 + lane[0:1], lcat, 0)
        start = pl.multiple_of((l * BANDS + j) * TP, 16)
        y = jnp.dot(xb[pl.ds(start, 9 * TP), :], lcat[0:KW, :], preferred_element_type=F32)
        total = jnp.zeros((TP, 128), F32)
        for rr in range(9):
            w = tap_select(rr - 4 - o1, LAT_TAPS)
            total = total + w * y[rr * TP:(rr + 1) * TP]
        acc[lj] = total
        return 0

    with jax.named_scope("own"):
        lax.fori_loop(0, 32, own, 0)

    def square(first, step, total):
        for i in range(STEP):
            lj = 16 * (step // 2) + first + (4 if first else 12) * lax.rem(step, 2) + i
            a = acc[lj]
            total = jnp.where(lane == lj, jnp.sum(a * a, axis=1, keepdims=True), total)
        return total

    with jax.named_scope("square1"):
        total = lax.fori_loop(0, 4, lambda step, t: square(4, step, t), zero)

    for direction in range(2):
        def add(s, _):
            z_copy(direction, s).wait_recv()
            lj = (s // 4) * 16 + 12 * direction + lax.rem(s, 4)
            acc[lj] = acc[lj] + zr[direction, s]
            return 0

        def add_packed(c, _):
            z_copy(direction, c).wait_recv()
            z = zr[direction, c]
            hi = z.astype(BF16)
            both = jnp.concatenate([hi, (z - hi.astype(F32)).astype(BF16)], axis=0)
            start = pl.multiple_of(c * 128, 128)
            d = jnp.dot(both, spread[direction, pl.ds(start, 128), :], preferred_element_type=F32)
            for s in range(8):
                lj = (s // 4) * 16 + 12 * direction + s % 4
                acc[lj] = acc[lj] + (d[0:TP, s * 128:(s + 1) * 128] + d[TP:, s * 128:(s + 1) * 128])
            return 0

        @pl.when(has_down if direction else has_up)
        def _():
            with jax.named_scope("add"):
                lax.fori_loop(0, chunks, add if dense else add_packed, 0)

    with jax.named_scope("square2"):
        sums[0:TP, :] = lax.fori_loop(0, 4, lambda step, t: square(0, step, t), total)
    sums[TP:128, :] = jnp.zeros((128 - TP, 128), F32)
    row_sums = jnp.transpose(sums[...])[0:32]
    if not dense:
        flag = fs[...]
        for k, c in enumerate(f_copies):
            c.wait_recv()
            flag = flag + fr[k + 1]
        row_sums = jnp.where(lax.broadcasted_iota(jnp.int32, (32, 128), 1) >= FLAG, flag, row_sums)
    sums_t[...] = row_sums

    def exchange(peer, size, slots, send, recv, src):
        copies = []
        for k in range(1, size):
            copies.append(pltpu.make_async_remote_copy(
                src_ref=src, dst_ref=slots.at[k], send_sem=send.at[k], recv_sem=recv.at[k],
                device_id=peer(k), device_id_type=MESH))
        for c in copies:
            c.start()
        total = src[...]
        for k, c in enumerate(copies):
            c.wait_recv()
            total = total + slots[k + 1]
        return total, copies

    with jax.named_scope("exA"):
        total, a_copies = exchange(z_peer, ZGROUP, ra, a_send, a_recv, sums_t)
    ra[0] = total
    with jax.named_scope("exB"):
        total, b_copies = exchange(y_peer, ny * CORES, rb, b_send, b_recv, ra.at[0])
    flag_ref[...] = total[0:8]

    rms = jnp.sqrt(total * (1.0 / (128 * nlon)) + 1e-06)
    sums[0:32, 0:nt] = 1.0 + mask * (target_v[...] / rms[:, 0:nt] - 1.0)
    factor_t = jnp.transpose(sums[...])[0:TP]

    with jax.named_scope("scale"):
        for lj in range(32):
            out_ref[pl.ds(lj, nt, stride=32), :] = (acc[lj] * factor_t[:, lj:lj + 1])[0:nt]

    e_copy(0).wait_send()
    e_copy(1).wait_send()
    for c in a_copies + b_copies + f_copies:
        c.wait_send()
    for direction in range(2):
        @pl.when(has_up if direction else has_down)
        def _():
            o_copy(1 - direction).wait_send()
            lax.fori_loop(0, chunks, lambda s, _: (z_copy(direction, s).wait_send(), 0)[1], 0)


def solution(mesh):
    nlat, nlon = mesh.shape["lat"], mesh.shape["lon"]

    def body(tracers, offsets, target, band_mask):
        nt = tracers.shape[0]
        nb = nlon // ZGROUP
        vmem, dma = pltpu.VMEM, pltpu.SemaphoreType.DMA
        operands = (
            tracers.reshape(nt, 32, 128),
            offsets.reshape(64, 128),
            jnp.transpose(target, (1, 2, 0)).reshape(32, nt),
            band_mask,
        )

        def run(dense):
            return pl.pallas_call(
                functools.partial(kernel, dense, nt, nlat, nlon),
                out_shape=[jax.ShapeDtypeStruct((nt * 32, 128), F32), jax.ShapeDtypeStruct((8, 128), F32)],
                in_specs=[pl.BlockSpec(memory_space=pltpu.HBM)] * 4,
                out_specs=[pl.BlockSpec(memory_space=pltpu.VMEM)] * 2,
                scratch_shapes=[
                    vmem((TP * PITCH, 128), F32),
                    vmem((2 * BANDS * TP, KW), BF16),
                    vmem((64, 128), jnp.int32),
                    vmem((32, nt), F32),
                    pltpu.SMEM((16,), jnp.int32),
                    vmem((2, TP, 128), F32),
                    vmem((2, TP, 128), F32),
                    vmem((32, 128), jnp.int32),
                    vmem((2, 8, TP, 128), F32),
                    vmem((2, 8, TP, 128), F32),
                    vmem((32, TP, 128), F32),
                    vmem((2 * KW, 128), BF16),
                    vmem((128, 128), F32),
                    vmem((32, 128), F32),
                    vmem((ZGROUP, 32, 128), F32),
                    vmem((nb, 32, 128), F32),
                    vmem((1024, CAP), BF16),
                    vmem((2, CAP, 1024), BF16),
                    vmem((1, 128), F32),
                    vmem((nlat, 1, 128), F32),
                    dma((4,)), dma((2,)), dma((2,)), dma((2,)), dma((2,)), dma((2, 8)), dma((2, 8)),
                    dma((ZGROUP,)), dma((ZGROUP,)), dma((nb,)), dma((nb,)), dma((nlat,)), dma((nlat,)),
                ],
                compiler_params=pltpu.CompilerParams(
                    collective_id=int(dense), has_side_effects=True, vmem_limit_bytes=67043328
                ),
            )(*operands)

        out, flag = run(False)
        out = lax.cond(flag[0, FLAG] > 0.0, lambda: run(True)[0], lambda: out)
        return out.reshape(tracers.shape)

    placed = (
        P(None, None, "lat", "lon"),
        P(None, None, "lat", "lon"),
        P(None, None, "lat"),
        P("lat"),
    )
    return jax.shard_map(
        body, mesh=mesh, in_specs=placed, out_specs=P(None, None, "lat", "lon"), check_vma=False
    )
```

```python
import functools

import jax
import jax.numpy as jnp
from jax import lax
from jax.experimental import pallas as pl
from jax.experimental.pallas import tpu as pltpu
from jax.sharding import PartitionSpec as P

LON_TAPS = (-0.0546875, 0.8203125, 0.2734375, -0.0390625)
LAT_TAPS = (-0.0625, 0.5625, 0.5625, -0.0625)
MESH = pl.DeviceIdType.MESH
F32 = jnp.float32
BF16 = jnp.bfloat16
TP = 112
KW = 384
BANDS = 24
ZGROUP = 4
CORES = 2
PITCH = 40
STEP = 4
CAP = 512
BLOCK = 25
FLAG = 120


def tap_select(distance, taps):
    out = jnp.zeros(distance.shape, F32)
    for k in range(4):
        out = jnp.where(distance == k - 1, taps[k], out)
    return out


def lon_matrix(column, lcat, base, lanes=slice(0, 128), edges=True):
    rows = lax.broadcasted_iota(jnp.int32, (128, 128), 0)
    main = tap_select(rows - column, LON_TAPS).astype(BF16)
    lcat[base:base + 128, lanes] = main
    lcat[base + 128:base + 256, lanes] = main
    if edges:
        e = lax.broadcasted_iota(jnp.int32, (16, 128), 0) % 8
        edge = jnp.where(e < 4, e - 4, e + 124)
        lcat[base + 256:base + 272, lanes] = tap_select(edge - column, LON_TAPS).astype(BF16)


def places(o0, o1, direction):
    row = lax.broadcasted_iota(jnp.int32, (8, 128), 0)
    column = lax.broadcasted_iota(jnp.int32, (8, 128), 1) + o0
    reach = lax.rem(row, 4) + o1
    need = jnp.where(reach >= 2 if direction else reach <= 0, 1.0, 0.0)
    edge = jnp.where(column <= 0, need, 0.0) + jnp.where(column >= 126, need, 0.0)
    i = lax.broadcasted_iota(jnp.int32, (128, 128), 0)
    k = lax.broadcasted_iota(jnp.int32, (128, 128), 1)
    earlier = jnp.where(i < k, 1.0, 0.0).astype(BF16)
    both = jnp.concatenate([need - edge, edge], axis=0)
    before = jnp.dot(both.astype(BF16), earlier, preferred_element_type=F32)
    own = jnp.broadcast_to(jnp.sum(both, axis=1, keepdims=True), (16, 128))
    inner, outer, count = before[0:8], before[8:16], own[0:8] + own[8:16]
    for n in range(1, 8):
        a = jnp.where(row >= n, pltpu.roll(own[0:8], n, 0), 0.0)
        b = jnp.where(row >= n, pltpu.roll(own[8:16], n, 0), 0.0)
        inner, outer, count = inner + a, outer + b, count + (a + b)
    number = jnp.where(need > 0.0, jnp.where(edge > 0.0, CAP - 1.0 - outer, inner), -1.0)
    return number.astype(jnp.int32), count


def kernel(dense, nt, nlat, nlon, x_hbm, off_hbm, target_hbm, mask_hbm, adv_hbm, fac_hbm, flag_hbm,
           xv, xb, offv, target_v, mask_v, es, er, ob, zs, zr, acc, lcat, lpair, sums, factor, flag_v, ra, rb,
           known, pick, spread, fs, fr,
           local_sem, e_send, e_recv, o_send, o_recv, z_send, z_recv, a_send, a_recv, b_send, b_recv,
           f_send, f_recv, w_sem):
    lat = lax.axis_index("lat")
    lon = lax.axis_index("lon")
    left = lax.rem(lon + nlon - 1, nlon)
    right = lax.rem(lon + 1, nlon)
    core = lax.rem(lon, CORES)
    zlo = lax.rem(lon // CORES, ZGROUP)
    ny = nlon // (ZGROUP * CORES)
    yy = lon // (ZGROUP * CORES)
    chunks = 8 if dense else CAP // 128

    load_x = pltpu.make_async_copy(
        x_hbm, xv.reshape(TP, PITCH, 128).at[pl.ds(0, nt), pl.ds(0, 32), :], local_sem.at[0])
    load_x.start()
    load_off = pltpu.make_async_copy(off_hbm, offv, local_sem.at[1])
    load_off.start()
    load_target = pltpu.make_async_copy(target_hbm, target_v, local_sem.at[2])
    load_target.start()
    load_mask = pltpu.make_async_copy(mask_hbm, mask_v, local_sem.at[3])
    load_mask.start()

    def z_peer(k):
        return {"lon": (yy * ZGROUP + lax.rem(zlo + k, ZGROUP)) * CORES + core}

    def y_peer(k):
        me = yy * CORES + core
        other = lax.rem(me + k, ny * CORES)
        return {"lon": ((other // CORES) * ZGROUP + zlo) * CORES + lax.rem(other, CORES)}

    def x_peer(k):
        return {"lat": lax.rem(lat + 2 * k, nlat)}

    barrier = pltpu.get_barrier_semaphore()

    def greet(device):
        pl.semaphore_signal(barrier, inc=1, device_id=device, device_id_type=MESH)

    has_up = lat > 0
    has_down = lat < nlat - 1

    @pl.when(has_up)
    def _():
        greet({"lat": lat - 1})

    @pl.when(has_down)
    def _():
        greet({"lat": lat + 1})

    for k in range(1, nlat // 2):
        greet(x_peer(k))
    greet({"lon": left})
    greet({"lon": right})
    for k in range(1, ZGROUP):
        greet(z_peer(k))
    for k in range(1, ny * CORES):
        greet(y_peer(k))

    xv[pl.ds(nt * PITCH, (TP - nt) * PITCH), :] = jnp.zeros(((TP - nt) * PITCH, 128), F32)
    for l in range(2):
        for first in (0, 20):
            xb[pl.ds((l * BANDS + first) * TP, 4 * TP), :] = jnp.zeros((4 * TP, KW), BF16)
        lcat[l * KW + 272:(l + 1) * KW, :] = jnp.zeros((112, 128), BF16)
    lpair[272:KW, :] = jnp.zeros((112, 256), BF16)
    lane = lax.broadcasted_iota(jnp.int32, (TP, 128), 1)

    load_off.wait()
    with jax.named_scope("barw"):
        pl.semaphore_wait(
            barrier,
            has_up.astype(jnp.int32) + has_down.astype(jnp.int32) + nlat // 2 + 1 + (ZGROUP - 1) + (ny * CORES - 1))

    ob4 = ob.reshape(2, 2, 2, 4, 128)

    def o_copy(direction):
        return pltpu.make_async_remote_copy(
            src_ref=offv.reshape(2, 2, 16, 128).at[:, :, pl.ds(12 * direction, 4), :],
            dst_ref=ob4.at[direction],
            send_sem=o_send.at[direction], recv_sem=o_recv.at[direction],
            device_id={"lat": lat - 1 + 2 * direction}, device_id_type=MESH)

    @pl.when(has_up)
    def _():
        o_copy(0).start()

    @pl.when(has_down)
    def _():
        o_copy(1).start()

    load_x.wait()

    group = lane // 4

    def pack(step, carry):
        to_left, to_right = carry
        for i in range(STEP):
            lj = step * STEP + i
            v = xv[pl.ds(lj, TP, stride=PITCH), :]
            rolled = pltpu.roll(v, 4 * lj, 1)
            to_left = jnp.where(group == lj, rolled, to_left)
            to_right = jnp.where(group == lax.rem(lj + 31, 32), rolled, to_right)
            hi = v.astype(BF16)
            lo = (v - hi.astype(F32)).astype(BF16)
            row = pl.multiple_of(((lj // 16) * BANDS + 4 + lax.rem(lj, 16)) * TP, 16)
            xb[pl.ds(row, TP), 0:128] = hi
            xb[pl.ds(row, TP), 128:256] = lo
        return to_left, to_right

    zero = jnp.zeros((TP, 128), F32)
    with jax.named_scope("pack"):
        to_left, to_right = lax.fori_loop(0, 32 // STEP, pack, (zero, zero))
    es[0] = to_left
    es[1] = to_right

    def e_copy(side):
        return pltpu.make_async_remote_copy(
            src_ref=es.at[side], dst_ref=er.at[1 - side],
            send_sem=e_send.at[side], recv_sem=e_recv.at[1 - side],
            device_id={"lon": left if side == 0 else right}, device_id_type=MESH)

    def z_copy(direction, s):
        return pltpu.make_async_remote_copy(
            src_ref=zs.at[direction, s, pl.ds(0, nt)], dst_ref=zr.at[direction, s, pl.ds(0, nt)],
            send_sem=z_send.at[direction, s], recv_sem=z_recv.at[direction, s],
            device_id={"lat": lat + 1 - 2 * direction}, device_id_type=MESH)

    e_copy(0).start()
    e_copy(1).start()

    f_copies = []
    place = []
    if not dense:
        flag = jnp.zeros((8, 128), F32)
        for direction in range(2):
            o0, o1 = [
                jnp.concatenate([offv[pl.ds(first + 12 * direction, 4), :], offv[pl.ds(first + 16 + 12 * direction, 4), :]], axis=0)
                for first in (0, 32)
            ]
            p, count = places(o0, o1, direction)
            place.append(p)
            exists = has_up if direction == 0 else has_down
            flag = jnp.maximum(flag, jnp.where(count > CAP, exists.astype(F32), 0.0))
        fs[0] = jnp.broadcast_to(jnp.max(flag, axis=(0, 1), keepdims=True), (1, 128))
        for k in range(nlat // 2):
            f_copies.append(pltpu.make_async_remote_copy(
                src_ref=fs.at[min(k, 1)], dst_ref=fr.at[k], send_sem=f_send.at[k], recv_sem=f_recv.at[k],
                device_id=x_peer(k) if k else {"lat": lat + 1 - 2 * lax.rem(lat, 2)}, device_id_type=MESH))
        f_copies[0].start()

    def edges(first, step):
        for i in range(STEP):
            lj = 16 * (step // 2) + first + (4 if first else 12) * lax.rem(step, 2) + i
            shift = lax.rem(132 - 4 * lj, 128)
            a = pltpu.roll(er[0], shift, 1)
            b = pltpu.roll(er[1], shift, 1)
            e = jnp.where(lane < 4, a, b)
            hi = e.astype(BF16).astype(F32)
            both = jnp.where(lane < 8, hi, pltpu.roll(e - hi, 8, 1))
            row = pl.multiple_of(((lj // 16) * BANDS + 4 + lax.rem(lj, 16)) * TP, 16)
            xb[pl.ds(row, TP), 256:384] = both.astype(BF16)
        return 0

    def send_dense(direction):
        def part(s, _):
            l, jj = s // 4, lax.rem(s, 4)
            o0 = ob[pl.ds(16 * direction + s, 1), :]
            o1 = ob[pl.ds(16 * direction + 8 + s, 1), :]
            lon_matrix(o0 + lane[0:1], lcat, 0)
            start = pl.multiple_of((l * BANDS + 4 + 12 * (1 - direction)) * TP, 16)
            y = jnp.dot(xb[pl.ds(start, 4 * TP), :], lcat[0:KW, :], preferred_element_type=F32)
            total = jnp.zeros((TP, 128), F32)
            for hh in range(4):
                w = tap_select(hh + (4 if direction else -4) - jj - o1, LAT_TAPS)
                total = total + w * y[hh * TP:(hh + 1) * TP]
            zs[direction, s] = total
            z_copy(direction, s).start()
            return 0

        lax.fori_loop(0, 8, part, 0)

    def find_cells(direction):
        o0 = ob[pl.ds(16 * direction, 8), :]
        o1 = ob[pl.ds(16 * direction + 8, 8), :]
        row = lax.broadcasted_iota(jnp.int32, (8, 128), 0)
        column = lax.broadcasted_iota(jnp.int32, (8, 128), 1) + o0
        reach = lax.rem(row, 4) + o1
        number, _ = places(o0, o1, direction)
        number_t = jnp.transpose(jnp.concatenate([number, jnp.zeros((120, 128), jnp.int32)], axis=0))
        slot = lax.broadcasted_iota(jnp.int32, (128, CAP), 1)
        row16 = lax.broadcasted_iota(jnp.int32, (16, 128), 0)
        cells = []
        for s in range(8):
            pick[s * 128:(s + 1) * 128, :] = jnp.where(number_t[:, s:s + 1] == slot, 1.0, 0.0).astype(BF16)
            v = jnp.where(row16 == 0, column[s:s + 1], jnp.where(row16 == 1, reach[s:s + 1], s // 4))
            cells.append(v.astype(F32).astype(BF16))
        found = jnp.dot(jnp.concatenate(cells, axis=1), pick[...], preferred_element_type=F32)
        known[direction] = found.astype(jnp.int32)

    def send_packed(direction, c, with_edges):
        here = slice(c * 128, (c + 1) * 128)
        column, reach, level = [known[direction, k:k + 1, here] for k in range(3)]
        depth = KW if with_edges else 256
        y = jnp.zeros((4 * TP, 128), F32)
        for l in range(2):
            lon_matrix(jnp.where(level == l, column, 4096), lcat, l * KW, edges=with_edges)
            start = (l * BANDS + 4 + 12 * (1 - direction)) * TP
            y = y + jnp.dot(
                xb[start:start + 4 * TP, 0:depth], lcat[l * KW:l * KW + depth, :], preferred_element_type=F32)
        total = jnp.zeros((TP, 128), F32)
        for hh in range(4):
            w = tap_select(hh + (4 if direction else -4) - reach, LAT_TAPS)
            total = total + w * y[hh * TP:(hh + 1) * TP]
        zs[direction, c] = total
        z_copy(direction, c).start()

    if dense:
        with jax.named_scope("ewait"):
            for side in range(2):
                pltpu.make_async_remote_copy(
                    src_ref=es.at[side], dst_ref=er.at[side], send_sem=e_send.at[side], recv_sem=e_recv.at[side],
                    device_id={"lon": left}, device_id_type=MESH).wait_recv()

        with jax.named_scope("edges"):
            lax.fori_loop(0, 4, lambda step, _: edges(0, step), 0)

    for direction in range(2):
        @pl.when(has_up if direction else has_down)
        def _():
            with jax.named_scope("owait"):
                pltpu.make_async_remote_copy(
                    src_ref=ob4.at[direction], dst_ref=ob4.at[direction],
                    send_sem=o_send.at[direction], recv_sem=o_recv.at[direction],
                    device_id={"lat": lat + 1 - 2 * direction}, device_id_type=MESH).wait_recv()
            with jax.named_scope("part"):
                if dense:
                    send_dense(direction)
                else:
                    find_cells(direction)
                    for c in range(CAP // 128 - 1):
                        send_packed(direction, c, False)

    if not dense:
        with jax.named_scope("ewait"):
            for side in range(2):
                pltpu.make_async_remote_copy(
                    src_ref=es.at[side], dst_ref=er.at[side], send_sem=e_send.at[side], recv_sem=e_recv.at[side],
                    device_id={"lon": left}, device_id_type=MESH).wait_recv()

        with jax.named_scope("edges"):
            lax.fori_loop(0, 4, lambda step, _: edges(0, step), 0)

        for direction in range(2):
            @pl.when(has_up if direction else has_down)
            def _():
                with jax.named_scope("part_edges"):
                    send_packed(direction, CAP // 128 - 1, True)

        slot = lax.broadcasted_iota(jnp.int32, (CAP, 128), 0)
        with jax.named_scope("spread"):
            for direction in range(2):
                for s in range(8):
                    spread[direction, :, s * 128:(s + 1) * 128] = jnp.where(
                        place[direction][s:s + 1] == slot, 1.0, 0.0).astype(BF16)

        f_copies[0].wait_recv()
        fs[1] = fs[0] + fr[0]
        for c in f_copies[1:]:
            c.start()

    with jax.named_scope("edges2"):
        lax.fori_loop(0, 4, lambda step, _: edges(4, step), 0)

    def own(pair, _):
        l, j = pair // 8, 2 * lax.rem(pair, 8)
        lj = 16 * l + j
        for i in range(2):
            lon_matrix(offv[pl.ds(lj + i, 1), :] + lane[0:1], lpair, 0, slice(128 * i, 128 * i + 128))
        start = pl.multiple_of((l * BANDS + j) * TP, 16)
        y = jnp.dot(xb[pl.ds(start, 10 * TP), :], lpair[...], preferred_element_type=F32)
        for i in range(2):
            o1 = offv[pl.ds(32 + lj + i, 1), :]
            total = jnp.zeros((TP, 128), F32)
            for rr in range(9):
                w = tap_select(rr - 4 - o1, LAT_TAPS)
                total = total + w * y[(rr + i) * TP:(rr + i + 1) * TP, 128 * i:128 * i + 128]
            acc[lj + i] = total
        return 0

    with jax.named_scope("own"):
        lax.fori_loop(0, 16, own, 0)

    def square(first, step, total):
        for i in range(STEP):
            a = acc[16 * (step // 2) + first + (4 if first else 12) * lax.rem(step, 2) + i]
            total = jnp.where(lane == 4 * step + i, jnp.sum(a * a, axis=1, keepdims=True), total)
        return total

    def row_sums(first):
        sums[0:TP, :] = lax.fori_loop(0, 4, lambda step, t: square(first, step, t), zero)
        sums[TP:128, :] = jnp.zeros((128 - TP, 128), F32)
        return jnp.transpose(sums[...])[0:16]

    def exchange(peer, size, slots, send, recv):
        return [
            pltpu.make_async_remote_copy(
                src_ref=slots.at[0], dst_ref=slots.at[k], send_sem=send.at[k], recv_sem=recv.at[k],
                device_id=peer(k), device_id_type=MESH)
            for k in range(1, size)
        ]

    def total_of(copies, slots):
        total = slots[0]
        for k, c in enumerate(copies):
            c.wait_recv()
            total = total + slots[k + 1]
        return total

    a_copies = [exchange(z_peer, ZGROUP, ra.at[n], a_send.at[n], a_recv.at[n]) for n in range(2)]
    b_copies = [exchange(y_peer, ny * CORES, rb.at[n], b_send.at[n], b_recv.at[n]) for n in range(2)]

    with jax.named_scope("square1"):
        inner = row_sums(4)
    if not dense:
        flag = fs[1]
        for k, c in enumerate(f_copies[1:]):
            c.wait_recv()
            flag = flag + fr[k + 1]
        inner = jnp.where(lax.broadcasted_iota(jnp.int32, (16, 128), 1) >= FLAG, flag, inner)
    ra[0, 0] = inner
    for c in a_copies[0]:
        c.start()

    def save(lj):
        return pltpu.make_async_copy(acc.at[lj, pl.ds(0, nt)], adv_hbm.at[:, lj], w_sem.at[lj])

    def save_rows(first):
        def one(k, _):
            save(16 * (k // 8) + (lax.rem(k, 8) + 4 if first else lax.rem(k, 8) + 8 * (lax.rem(k, 8) // 4))).start()
            return 0

        lax.fori_loop(0, 16, one, 0)

    save_rows(4)

    def add(direction, c):
        z_copy(direction, c).wait_recv()
        z = zr[direction, c]
        if dense:
            lj = (c // 4) * 16 + 12 * direction + lax.rem(c, 4)
            acc[lj] = acc[lj] + z
            return
        hi = z.astype(BF16)
        both = jnp.concatenate([hi, (z - hi.astype(F32)).astype(BF16)], axis=0)
        start = pl.multiple_of(c * 128, 128)
        d = jnp.dot(both, spread[direction, pl.ds(start, 128), :], preferred_element_type=F32)
        for s in range(8):
            lj = (s // 4) * 16 + 12 * direction + s % 4
            acc[lj] = acc[lj] + (d[0:TP, s * 128:(s + 1) * 128] + d[TP:, s * 128:(s + 1) * 128])

    def add_both(c, _):
        for direction in range(2):
            @pl.when(has_down if direction else has_up)
            def _():
                add(direction, c)
        return 0

    with jax.named_scope("add"):
        lax.fori_loop(0, chunks - 1, add_both, 0)
    with jax.named_scope("exA1"):
        rb[0, 0] = total_of(a_copies[0], ra.at[0])
        for c in b_copies[0]:
            c.start()
    with jax.named_scope("add_last"):
        add_both(chunks - 1, 0)

    with jax.named_scope("square2"):
        ra[1, 0] = row_sums(0)
    for c in a_copies[1]:
        c.start()
    save_rows(0)
    with jax.named_scope("exA"):
        rb[1, 0] = total_of(a_copies[1], ra.at[1])
    for c in b_copies[1]:
        c.start()
    with jax.named_scope("exB1"):
        inner = total_of(b_copies[0], rb.at[0])
    flag_v[0] = jnp.where(jnp.max(inner[0:8, FLAG:128]) > 0.0, 1, 0)
    put_flag = pltpu.make_async_copy(flag_v, flag_hbm, local_sem.at[0])
    put_flag.start()
    load_target.wait()
    load_mask.wait()
    row = lax.rem(lax.broadcasted_iota(jnp.int32, (32, 128), 0), 16)
    mask = jnp.zeros((32, 128), F32)
    for j in range(16):
        mask = jnp.where(row == j, mask_v[j].astype(F32) * 0.5, mask)
    with jax.named_scope("exB"):
        outer = total_of(b_copies[1], rb.at[1])
    for l in range(2):
        sums[16 * l:16 * l + 4, :] = outer[8 * l:8 * l + 4]
        sums[16 * l + 4:16 * l + 12, :] = inner[8 * l:8 * l + 8]
        sums[16 * l + 12:16 * l + 16, :] = outer[8 * l + 4:8 * l + 8]
    rms = jnp.sqrt(sums[0:32, :] * (1.0 / (128 * nlon)) + 1e-06)
    factor[:, 0:nt] = 1.0 + mask[:, 0:nt] * (target_v[...] / rms[:, 0:nt] - 1.0)
    put_factor = pltpu.make_async_copy(factor, fac_hbm, local_sem.at[1])
    put_factor.start()

    lax.fori_loop(0, 32, lambda lj, _: (save(lj).wait(), 0)[1], 0)
    e_copy(0).wait_send()
    e_copy(1).wait_send()
    for c in a_copies[0] + a_copies[1] + b_copies[0] + b_copies[1] + f_copies:
        c.wait_send()
    for direction in range(2):
        @pl.when(has_up if direction else has_down)
        def _():
            o_copy(1 - direction).wait_send()
            lax.fori_loop(0, chunks, lambda s, _: (z_copy(direction, s).wait_send(), 0)[1], 0)
    put_flag.wait()
    put_factor.wait()


def scale(fac_hbm, adv_hbm, out_hbm, fac_v, rows_v, in_sem, out_sem, fac_sem):
    size = BLOCK * 32
    parts = rows_v.shape[0]
    load_fac = pltpu.make_async_copy(fac_hbm, fac_v, fac_sem)
    load_fac.start()
    loads = [pltpu.make_async_copy(adv_hbm.at[pl.ds(size * n, size)], rows_v.at[n], in_sem.at[n]) for n in range(parts)]
    stores = [pltpu.make_async_copy(rows_v.at[n], out_hbm.at[pl.ds(size * n, size)], out_sem.at[n]) for n in range(parts)]
    for c in loads:
        c.start()
    load_fac.wait()
    for n in range(parts):
        loads[n].wait()
        for t in range(BLOCK):
            here = slice(32 * t, 32 * t + 32)
            column = BLOCK * n + t
            rows_v[n, here, :] = rows_v[n, here, :] * fac_v[:, column:column + 1]
        stores[n].start()
    for c in stores:
        c.wait()


def solution(mesh):
    nlat, nlon = mesh.shape["lat"], mesh.shape["lon"]

    def body(tracers, offsets, target, band_mask):
        nt = tracers.shape[0]
        nb = nlon // ZGROUP
        vmem, dma = pltpu.VMEM, pltpu.SemaphoreType.DMA
        operands = (
            tracers.reshape(nt, 32, 128),
            offsets.reshape(64, 128),
            jnp.transpose(target, (1, 2, 0)).reshape(32, nt),
            band_mask,
        )

        def run(dense):
            return pl.pallas_call(
                functools.partial(kernel, dense, nt, nlat, nlon),
                out_shape=[
                    jax.ShapeDtypeStruct((nt, 32, 128), F32),
                    jax.ShapeDtypeStruct((32, 128), F32),
                    jax.ShapeDtypeStruct((1,), jnp.int32),
                ],
                in_specs=[pl.BlockSpec(memory_space=pltpu.HBM)] * 4,
                out_specs=[pl.BlockSpec(memory_space=pltpu.HBM)] * 3,
                scratch_shapes=[
                    vmem((TP * PITCH, 128), F32),
                    vmem((2 * BANDS * TP, KW), BF16),
                    vmem((64, 128), jnp.int32),
                    vmem((32, nt), F32),
                    pltpu.SMEM((16,), jnp.int32),
                    vmem((2, TP, 128), F32),
                    vmem((2, TP, 128), F32),
                    vmem((32, 128), jnp.int32),
                    vmem((2, 8, TP, 128), F32),
                    vmem((2, 8, TP, 128), F32),
                    vmem((32, TP, 128), F32),
                    vmem((2 * KW, 128), BF16),
                    vmem((KW, 256), BF16),
                    vmem((128, 128), F32),
                    vmem((32, 128), F32),
                    pltpu.SMEM((1,), jnp.int32),
                    vmem((2, ZGROUP, 16, 128), F32),
                    vmem((2, nb, 16, 128), F32),
                    vmem((2, 16, CAP), jnp.int32),
                    vmem((1024, CAP), BF16),
                    vmem((2, CAP, 1024), BF16),
                    vmem((2, 1, 128), F32),
                    vmem((nlat // 2, 1, 128), F32),
                    dma((4,)), dma((2,)), dma((2,)), dma((2,)), dma((2,)), dma((2, 8)), dma((2, 8)),
                    dma((2, ZGROUP)), dma((2, ZGROUP)), dma((2, nb)), dma((2, nb)), dma((nlat // 2,)), dma((nlat // 2,)), dma((32,)),
                ],
                compiler_params=pltpu.CompilerParams(
                    collective_id=int(dense), has_side_effects=True, vmem_limit_bytes=67043328
                ),
            )(*operands)

        adv, fac, flag = run(False)
        adv, fac = lax.cond(flag[0] > 0, lambda: tuple(run(True)[0:2]), lambda: (adv, fac))
        out = pl.pallas_call(
            scale,
            out_shape=jax.ShapeDtypeStruct((nt * 32, 128), F32),
            in_specs=[pl.BlockSpec(memory_space=pltpu.HBM)] * 2,
            out_specs=pl.BlockSpec(memory_space=pltpu.HBM),
            scratch_shapes=[
                vmem((32, 128), F32), vmem((nt // BLOCK, BLOCK * 32, 128), F32), dma((nt // BLOCK,)), dma((nt // BLOCK,)), dma,
            ],
            compiler_params=pltpu.CompilerParams(vmem_limit_bytes=67043328),
        )(fac, adv.reshape(nt * 32, 128))
        return out.reshape(tracers.shape)

    placed = (
        P(None, None, "lat", "lon"),
        P(None, None, "lat", "lon"),
        P(None, None, "lat"),
        P("lat"),
    )
    return jax.shard_map(
        body, mesh=mesh, in_specs=placed, out_specs=P(None, None, "lat", "lon"), check_vma=False
    )
```

```python
import functools

import jax
import jax.numpy as jnp
from jax import lax
from jax.experimental import pallas as pl
from jax.experimental.pallas import tpu as pltpu
from jax.sharding import PartitionSpec as P

LON_TAPS = (-0.0546875, 0.8203125, 0.2734375, -0.0390625)
LAT_TAPS = (-0.0625, 0.5625, 0.5625, -0.0625)
MESH = pl.DeviceIdType.MESH
F32 = jnp.float32
BF16 = jnp.bfloat16
TP = 112
KW = 384
BANDS = 24
ZGROUP = 4
CORES = 2
PITCH = 40
STEP = 4
CAP = 512
FLAG = 120


def tap_select(distance, taps):
    out = jnp.zeros(distance.shape, F32)
    for k in range(4):
        out = jnp.where(distance == k - 1, taps[k], out)
    return out


def lon_matrix(column, lcat, base, lanes=slice(0, 128), edges=True):
    rows = lax.broadcasted_iota(jnp.int32, (128, 128), 0)
    main = tap_select(rows - column, LON_TAPS).astype(BF16)
    lcat[base:base + 128, lanes] = main
    lcat[base + 128:base + 256, lanes] = main
    if edges:
        e = lax.broadcasted_iota(jnp.int32, (16, 128), 0) % 8
        edge = jnp.where(e < 4, e - 4, e + 124)
        lcat[base + 256:base + 272, lanes] = tap_select(edge - column, LON_TAPS).astype(BF16)


def places(o0, o1, direction):
    row = lax.broadcasted_iota(jnp.int32, (8, 128), 0)
    column = lax.broadcasted_iota(jnp.int32, (8, 128), 1) + o0
    reach = lax.rem(row, 4) + o1
    need = jnp.where(reach >= 2 if direction else reach <= 0, 1.0, 0.0)
    edge = jnp.where(column <= 0, need, 0.0) + jnp.where(column >= 126, need, 0.0)
    i = lax.broadcasted_iota(jnp.int32, (128, 128), 0)
    k = lax.broadcasted_iota(jnp.int32, (128, 128), 1)
    earlier = jnp.where(i < k, 1.0, 0.0).astype(BF16)
    both = jnp.concatenate([need - edge, edge], axis=0)
    before = jnp.dot(both.astype(BF16), earlier, preferred_element_type=F32)
    own = jnp.broadcast_to(jnp.sum(both, axis=1, keepdims=True), (16, 128))
    inner, outer, count = before[0:8], before[8:16], own[0:8] + own[8:16]
    for n in range(1, 8):
        a = jnp.where(row >= n, pltpu.roll(own[0:8], n, 0), 0.0)
        b = jnp.where(row >= n, pltpu.roll(own[8:16], n, 0), 0.0)
        inner, outer, count = inner + a, outer + b, count + (a + b)
    number = jnp.where(need > 0.0, jnp.where(edge > 0.0, CAP - 1.0 - outer, inner), -1.0)
    return number.astype(jnp.int32), count


def kernel(dense, nt, nlat, nlon, x_hbm, off_hbm, target_hbm, mask_hbm, out_ref, flag_hbm,
           xv, xb, offv, target_v, mask_v, es, er, ob, zs, zr, acc, lcat, lpair, sums, flag_v, ra, rb,
           known, pick, spread, fs, fr,
           local_sem, e_send, e_recv, o_send, o_recv, z_send, z_recv, a_send, a_recv, b_send, b_recv,
           f_send, f_recv):
    lat = lax.axis_index("lat")
    lon = lax.axis_index("lon")
    left = lax.rem(lon + nlon - 1, nlon)
    right = lax.rem(lon + 1, nlon)
    core = lax.rem(lon, CORES)
    zlo = lax.rem(lon // CORES, ZGROUP)
    ny = nlon // (ZGROUP * CORES)
    yy = lon // (ZGROUP * CORES)
    chunks = 8 if dense else CAP // 128

    load_x = pltpu.make_async_copy(
        x_hbm, xv.reshape(TP, PITCH, 128).at[pl.ds(0, nt), pl.ds(0, 32), :], local_sem.at[0])
    load_x.start()
    load_off = pltpu.make_async_copy(off_hbm, offv, local_sem.at[1])
    load_off.start()
    load_target = pltpu.make_async_copy(target_hbm, target_v, local_sem.at[2])
    load_target.start()
    load_mask = pltpu.make_async_copy(mask_hbm, mask_v, local_sem.at[3])
    load_mask.start()

    def z_peer(k):
        return {"lon": (yy * ZGROUP + lax.rem(zlo + k, ZGROUP)) * CORES + core}

    def y_peer(k):
        me = yy * CORES + core
        other = lax.rem(me + k, ny * CORES)
        return {"lon": ((other // CORES) * ZGROUP + zlo) * CORES + lax.rem(other, CORES)}

    def x_peer(k):
        return {"lat": lax.rem(lat + 2 * k, nlat)}

    barrier = pltpu.get_barrier_semaphore()

    def greet(device):
        pl.semaphore_signal(barrier, inc=1, device_id=device, device_id_type=MESH)

    has_up = lat > 0
    has_down = lat < nlat - 1

    @pl.when(has_up)
    def _():
        greet({"lat": lat - 1})

    @pl.when(has_down)
    def _():
        greet({"lat": lat + 1})

    for k in range(1, nlat // 2):
        greet(x_peer(k))
    greet({"lon": left})
    greet({"lon": right})
    for k in range(1, ZGROUP):
        greet(z_peer(k))
    for k in range(1, ny * CORES):
        greet(y_peer(k))

    xv[pl.ds(nt * PITCH, (TP - nt) * PITCH), :] = jnp.zeros(((TP - nt) * PITCH, 128), F32)
    for l in range(2):
        for first in (0, 20):
            xb[pl.ds((l * BANDS + first) * TP, 4 * TP), :] = jnp.zeros((4 * TP, KW), BF16)
        lcat[l * KW + 272:(l + 1) * KW, :] = jnp.zeros((112, 128), BF16)
    lpair[272:KW, :] = jnp.zeros((112, 256), BF16)
    lane = lax.broadcasted_iota(jnp.int32, (TP, 128), 1)

    load_off.wait()
    with jax.named_scope("barw"):
        pl.semaphore_wait(
            barrier,
            has_up.astype(jnp.int32) + has_down.astype(jnp.int32) + nlat // 2 + 1 + (ZGROUP - 1) + (ny * CORES - 1))

    ob4 = ob.reshape(2, 2, 2, 4, 128)

    def o_copy(direction):
        return pltpu.make_async_remote_copy(
            src_ref=offv.reshape(2, 2, 16, 128).at[:, :, pl.ds(12 * direction, 4), :],
            dst_ref=ob4.at[direction],
            send_sem=o_send.at[direction], recv_sem=o_recv.at[direction],
            device_id={"lat": lat - 1 + 2 * direction}, device_id_type=MESH)

    @pl.when(has_up)
    def _():
        o_copy(0).start()

    @pl.when(has_down)
    def _():
        o_copy(1).start()

    load_x.wait()

    group = lane // 4

    def pack(step, carry):
        to_left, to_right = carry
        for i in range(STEP):
            lj = step * STEP + i
            v = xv[pl.ds(lj, TP, stride=PITCH), :]
            rolled = pltpu.roll(v, 4 * lj, 1)
            to_left = jnp.where(group == lj, rolled, to_left)
            to_right = jnp.where(group == lax.rem(lj + 31, 32), rolled, to_right)
            hi = v.astype(BF16)
            lo = (v - hi.astype(F32)).astype(BF16)
            row = pl.multiple_of(((lj // 16) * BANDS + 4 + lax.rem(lj, 16)) * TP, 16)
            xb[pl.ds(row, TP), 0:128] = hi
            xb[pl.ds(row, TP), 128:256] = lo
        return to_left, to_right

    zero = jnp.zeros((TP, 128), F32)
    with jax.named_scope("pack"):
        to_left, to_right = lax.fori_loop(0, 32 // STEP, pack, (zero, zero))
    es[0] = to_left
    es[1] = to_right

    def e_copy(side):
        return pltpu.make_async_remote_copy(
            src_ref=es.at[side, pl.ds(0, nt)], dst_ref=er.at[1 - side, pl.ds(0, nt)],
            send_sem=e_send.at[side], recv_sem=e_recv.at[1 - side],
            device_id={"lon": left if side == 0 else right}, device_id_type=MESH)

    def z_copy(direction, s):
        return pltpu.make_async_remote_copy(
            src_ref=zs.at[direction, s, pl.ds(0, nt)], dst_ref=zr.at[direction, s, pl.ds(0, nt)],
            send_sem=z_send.at[direction, s], recv_sem=z_recv.at[direction, s],
            device_id={"lat": lat + 1 - 2 * direction}, device_id_type=MESH)

    e_copy(0).start()
    e_copy(1).start()

    f_copies = []
    place = []
    if not dense:
        flag = jnp.zeros((8, 128), F32)
        for direction in range(2):
            o0, o1 = [
                jnp.concatenate([offv[pl.ds(first + 12 * direction, 4), :], offv[pl.ds(first + 16 + 12 * direction, 4), :]], axis=0)
                for first in (0, 32)
            ]
            p, count = places(o0, o1, direction)
            place.append(p)
            exists = has_up if direction == 0 else has_down
            flag = jnp.maximum(flag, jnp.where(count > CAP, exists.astype(F32), 0.0))
        fs[0] = jnp.broadcast_to(jnp.max(flag, axis=(0, 1), keepdims=True), (1, 128))
        for k in range(nlat // 2):
            f_copies.append(pltpu.make_async_remote_copy(
                src_ref=fs.at[min(k, 1)], dst_ref=fr.at[k], send_sem=f_send.at[k], recv_sem=f_recv.at[k],
                device_id=x_peer(k) if k else {"lat": lat + 1 - 2 * lax.rem(lat, 2)}, device_id_type=MESH))
        f_copies[0].start()

    def edges(first, step):
        for i in range(STEP):
            lj = 16 * (step // 2) + first + (4 if first else 12) * lax.rem(step, 2) + i
            shift = lax.rem(132 - 4 * lj, 128)
            a = pltpu.roll(er[0], shift, 1)
            b = pltpu.roll(er[1], shift, 1)
            e = jnp.where(lane < 4, a, b)
            hi = e.astype(BF16).astype(F32)
            both = jnp.where(lane < 8, hi, pltpu.roll(e - hi, 8, 1))
            row = pl.multiple_of(((lj // 16) * BANDS + 4 + lax.rem(lj, 16)) * TP, 16)
            xb[pl.ds(row, TP), 256:384] = both.astype(BF16)
        return 0

    def send_dense(direction):
        def part(s, _):
            l, jj = s // 4, lax.rem(s, 4)
            o0 = ob[pl.ds(16 * direction + s, 1), :]
            o1 = ob[pl.ds(16 * direction + 8 + s, 1), :]
            lon_matrix(o0 + lane[0:1], lcat, 0)
            start = pl.multiple_of((l * BANDS + 4 + 12 * (1 - direction)) * TP, 16)
            y = jnp.dot(xb[pl.ds(start, 4 * TP), :], lcat[0:KW, :], preferred_element_type=F32)
            total = jnp.zeros((TP, 128), F32)
            for hh in range(4):
                w = tap_select(hh + (4 if direction else -4) - jj - o1, LAT_TAPS)
                total = total + w * y[hh * TP:(hh + 1) * TP]
            zs[direction, s] = total
            z_copy(direction, s).start()
            return 0

        lax.fori_loop(0, 8, part, 0)

    def find_cells(direction):
        o0 = ob[pl.ds(16 * direction, 8), :]
        o1 = ob[pl.ds(16 * direction + 8, 8), :]
        row = lax.broadcasted_iota(jnp.int32, (8, 128), 0)
        column = lax.broadcasted_iota(jnp.int32, (8, 128), 1) + o0
        reach = lax.rem(row, 4) + o1
        number, _ = places(o0, o1, direction)
        number_t = jnp.transpose(jnp.concatenate([number, jnp.zeros((120, 128), jnp.int32)], axis=0))
        slot = lax.broadcasted_iota(jnp.int32, (128, CAP), 1)
        row16 = lax.broadcasted_iota(jnp.int32, (16, 128), 0)
        cells = []
        for s in range(8):
            pick[s * 128:(s + 1) * 128, :] = jnp.where(number_t[:, s:s + 1] == slot, 1.0, 0.0).astype(BF16)
            v = jnp.where(row16 == 0, column[s:s + 1], jnp.where(row16 == 1, reach[s:s + 1], s // 4))
            cells.append(v.astype(F32).astype(BF16))
        found = jnp.dot(jnp.concatenate(cells, axis=1), pick[...], preferred_element_type=F32)
        known[direction] = found.astype(jnp.int32)

    def send_packed(direction, c, with_edges):
        here = slice(c * 128, (c + 1) * 128)
        column, reach, level = [known[direction, k:k + 1, here] for k in range(3)]
        depth = KW if with_edges else 256
        y = jnp.zeros((4 * TP, 128), F32)
        for l in range(2):
            lon_matrix(jnp.where(level == l, column, 4096), lcat, l * KW, edges=with_edges)
            start = (l * BANDS + 4 + 12 * (1 - direction)) * TP
            y = y + jnp.dot(
                xb[start:start + 4 * TP, 0:depth], lcat[l * KW:l * KW + depth, :], preferred_element_type=F32)
        total = jnp.zeros((TP, 128), F32)
        for hh in range(4):
            w = tap_select(hh + (4 if direction else -4) - reach, LAT_TAPS)
            total = total + w * y[hh * TP:(hh + 1) * TP]
        zs[direction, c] = total
        z_copy(direction, c).start()

    if dense:
        with jax.named_scope("ewait"):
            for side in range(2):
                pltpu.make_async_remote_copy(
                    src_ref=es.at[side, pl.ds(0, nt)], dst_ref=er.at[side, pl.ds(0, nt)], send_sem=e_send.at[side], recv_sem=e_recv.at[side],
                    device_id={"lon": left}, device_id_type=MESH).wait_recv()

        with jax.named_scope("edges"):
            lax.fori_loop(0, 4, lambda step, _: edges(0, step), 0)

    for direction in range(2):
        @pl.when(has_up if direction else has_down)
        def _():
            with jax.named_scope("owait"):
                pltpu.make_async_remote_copy(
                    src_ref=ob4.at[direction], dst_ref=ob4.at[direction],
                    send_sem=o_send.at[direction], recv_sem=o_recv.at[direction],
                    device_id={"lat": lat + 1 - 2 * direction}, device_id_type=MESH).wait_recv()
            with jax.named_scope("part"):
                if dense:
                    send_dense(direction)
                else:
                    find_cells(direction)
                    for c in range(CAP // 128 - 1):
                        send_packed(direction, c, False)

    if not dense:
        with jax.named_scope("ewait"):
            for side in range(2):
                pltpu.make_async_remote_copy(
                    src_ref=es.at[side, pl.ds(0, nt)], dst_ref=er.at[side, pl.ds(0, nt)], send_sem=e_send.at[side], recv_sem=e_recv.at[side],
                    device_id={"lon": left}, device_id_type=MESH).wait_recv()

        with jax.named_scope("edges"):
            lax.fori_loop(0, 4, lambda step, _: edges(0, step), 0)

        for direction in range(2):
            @pl.when(has_up if direction else has_down)
            def _():
                with jax.named_scope("part_edges"):
                    send_packed(direction, CAP // 128 - 1, True)

        slot = lax.broadcasted_iota(jnp.int32, (CAP, 128), 0)
        with jax.named_scope("spread"):
            for direction in range(2):
                for s in range(8):
                    spread[direction, :, s * 128:(s + 1) * 128] = jnp.where(
                        place[direction][s:s + 1] == slot, 1.0, 0.0).astype(BF16)

        f_copies[0].wait_recv()
        fs[1] = fs[0] + fr[0]
        for c in f_copies[1:]:
            c.start()

    with jax.named_scope("edges2"):
        lax.fori_loop(0, 4, lambda step, _: edges(4, step), 0)

    def own(pair, inner):
        q = lax.rem(pair, 4)
        l, j = pair // 4, 2 * q + (4 if inner else 8 * (q // 2))
        lj = 16 * l + j
        for i in range(2):
            lon_matrix(offv[pl.ds(lj + i, 1), :] + lane[0:1], lpair, 0, slice(128 * i, 128 * i + 128))
        start = pl.multiple_of((l * BANDS + j) * TP, 16)
        y = jnp.dot(xb[pl.ds(start, 10 * TP), :], lpair[...], preferred_element_type=F32)
        for i in range(2):
            o1 = offv[pl.ds(32 + lj + i, 1), :]
            total = jnp.zeros((TP, 128), F32)
            for rr in range(9):
                w = tap_select(rr - 4 - o1, LAT_TAPS)
                total = total + w * y[(rr + i) * TP:(rr + i + 1) * TP, 128 * i:128 * i + 128]
            acc[lj + i] = total
        return 0

    with jax.named_scope("own_inner"):
        lax.fori_loop(0, 8, lambda pair, _: own(pair, True), 0)

    def row_sums(first):
        total = zero
        for n in range(16):
            a = acc[16 * (n // 8) + first + (n % 8 if first else n % 8 + 8 * (n % 8 // 4))]
            total = jnp.where(lane == n, jnp.sum(a * a, axis=1, keepdims=True), total)
        sums[0:TP, :] = total
        sums[TP:128, :] = jnp.zeros((128 - TP, 128), F32)
        return jnp.transpose(sums[...])[0:16]

    def exchange(peer, size, slots, send, recv):
        return [
            pltpu.make_async_remote_copy(
                src_ref=slots.at[0], dst_ref=slots.at[k], send_sem=send.at[k], recv_sem=recv.at[k],
                device_id=peer(k), device_id_type=MESH)
            for k in range(1, size)
        ]

    def total_of(copies, slots):
        total = slots[0]
        for k, c in enumerate(copies):
            c.wait_recv()
            total = total + slots[k + 1]
        return total

    a_copies = [exchange(z_peer, ZGROUP, ra.at[n], a_send.at[n], a_recv.at[n]) for n in range(2)]
    b_copies = [exchange(y_peer, ny * CORES, rb.at[n], b_send.at[n], b_recv.at[n]) for n in range(2)]

    with jax.named_scope("square1"):
        inner = row_sums(4)
    if not dense:
        flag = fs[1]
        for k, c in enumerate(f_copies[1:]):
            c.wait_recv()
            flag = flag + fr[k + 1]
        inner = jnp.where(lax.broadcasted_iota(jnp.int32, (16, 128), 1) >= FLAG, flag, inner)
    ra[0, 0] = inner
    for c in a_copies[0]:
        c.start()

    def save_rows(first):
        for n in range(16):
            lj = 16 * (n // 8) + first + (n % 8 if first else n % 8 + 8 * (n % 8 // 4))
            out_ref[pl.ds(lj, nt, stride=32), :] = acc[lj, 0:nt]

    save_rows(4)

    with jax.named_scope("own_outer"):
        lax.fori_loop(0, 8, lambda pair, _: own(pair, False), 0)

    def add(direction, c):
        z_copy(direction, c).wait_recv()
        z = zr[direction, c]
        if dense:
            lj = (c // 4) * 16 + 12 * direction + lax.rem(c, 4)
            acc[lj] = acc[lj] + z
            return
        hi = z.astype(BF16)
        both = jnp.concatenate([hi, (z - hi.astype(F32)).astype(BF16)], axis=0)
        start = pl.multiple_of(c * 128, 128)
        d = jnp.dot(both, spread[direction, pl.ds(start, 128), :], preferred_element_type=F32)
        for s in range(8):
            lj = (s // 4) * 16 + 12 * direction + s % 4
            acc[lj] = acc[lj] + (d[0:TP, s * 128:(s + 1) * 128] + d[TP:, s * 128:(s + 1) * 128])

    def add_both(c, _):
        for direction in range(2):
            @pl.when(has_down if direction else has_up)
            def _():
                add(direction, c)
        return 0

    with jax.named_scope("add"):
        lax.fori_loop(0, chunks - 1, add_both, 0)
    with jax.named_scope("exA1"):
        rb[0, 0] = total_of(a_copies[0], ra.at[0])
        for c in b_copies[0]:
            c.start()
    with jax.named_scope("add_last"):
        add_both(chunks - 1, 0)

    with jax.named_scope("square2"):
        ra[1, 0] = row_sums(0)
    for c in a_copies[1]:
        c.start()
    save_rows(0)
    with jax.named_scope("exA"):
        rb[1, 0] = total_of(a_copies[1], ra.at[1])
    for c in b_copies[1]:
        c.start()
    with jax.named_scope("exB1"):
        inner = total_of(b_copies[0], rb.at[0])
    flag_v[0] = jnp.where(jnp.max(inner[0:8, FLAG:128]) > 0.0, 1, 0)
    put_flag = pltpu.make_async_copy(flag_v, flag_hbm, local_sem.at[0])
    put_flag.start()
    load_target.wait()
    load_mask.wait()
    row = lax.rem(lax.broadcasted_iota(jnp.int32, (32, 128), 0), 16)
    mask = jnp.zeros((32, 128), F32)
    for j in range(16):
        mask = jnp.where(row == j, mask_v[j].astype(F32) * 0.5, mask)
    with jax.named_scope("exB"):
        outer = total_of(b_copies[1], rb.at[1])
    for l in range(2):
        sums[16 * l:16 * l + 4, :] = outer[8 * l:8 * l + 4]
        sums[16 * l + 4:16 * l + 12, :] = inner[8 * l:8 * l + 8]
        sums[16 * l + 12:16 * l + 16, :] = outer[8 * l + 4:8 * l + 8]
    rms = jnp.sqrt(sums[0:32, :] * (1.0 / (128 * nlon)) + 1e-06)
    factor = 1.0 + mask[:, 0:nt] * (target_v[...] / rms[:, 0:nt] - 1.0)
    with jax.named_scope("scale"):
        for t in range(nt):
            here = slice(32 * t, 32 * t + 32)
            out_ref[here, :] = out_ref[here, :] * factor[:, t:t + 1]

    e_copy(0).wait_send()
    e_copy(1).wait_send()
    for c in a_copies[0] + a_copies[1] + b_copies[0] + b_copies[1] + f_copies:
        c.wait_send()
    for direction in range(2):
        @pl.when(has_up if direction else has_down)
        def _():
            o_copy(1 - direction).wait_send()
            lax.fori_loop(0, chunks, lambda s, _: (z_copy(direction, s).wait_send(), 0)[1], 0)
    put_flag.wait()


def solution(mesh):
    nlat, nlon = mesh.shape["lat"], mesh.shape["lon"]

    def body(tracers, offsets, target, band_mask):
        nt = tracers.shape[0]
        nb = nlon // ZGROUP
        vmem, dma = pltpu.VMEM, pltpu.SemaphoreType.DMA
        operands = tuple(pltpu.with_memory_space_constraint(a, pltpu.HBM) for a in (
            tracers.reshape(nt, 32, 128),
            offsets.reshape(64, 128),
            jnp.transpose(target, (1, 2, 0)).reshape(32, nt),
            band_mask,
        ))

        def run(dense):
            return pl.pallas_call(
                functools.partial(kernel, dense, nt, nlat, nlon),
                out_shape=[
                    jax.ShapeDtypeStruct((nt * 32, 128), F32),
                    jax.ShapeDtypeStruct((1,), jnp.int32),
                ],
                in_specs=[pl.BlockSpec(memory_space=pltpu.HBM)] * 4,
                out_specs=[pl.BlockSpec(memory_space=pltpu.VMEM), pl.BlockSpec(memory_space=pltpu.HBM)],
                scratch_shapes=[
                    vmem((TP * PITCH, 128), F32),
                    vmem((2 * BANDS * TP, KW), BF16),
                    vmem((64, 128), jnp.int32),
                    vmem((32, nt), F32),
                    pltpu.SMEM((16,), jnp.int32),
                    vmem((2, TP, 128), F32),
                    vmem((2, TP, 128), F32),
                    vmem((32, 128), jnp.int32),
                    vmem((2, 8, TP, 128), F32),
                    vmem((2, 8, TP, 128), F32),
                    vmem((32, TP, 128), F32),
                    vmem((2 * KW, 128), BF16),
                    vmem((KW, 256), BF16),
                    vmem((128, 128), F32),
                    pltpu.SMEM((1,), jnp.int32),
                    vmem((2, ZGROUP, 16, 128), F32),
                    vmem((2, nb, 16, 128), F32),
                    vmem((2, 16, CAP), jnp.int32),
                    vmem((1024, CAP), BF16),
                    vmem((2, CAP, 1024), BF16),
                    vmem((2, 1, 128), F32),
                    vmem((nlat // 2, 1, 128), F32),
                    dma((4,)), dma((2,)), dma((2,)), dma((2,)), dma((2,)), dma((2, 8)), dma((2, 8)),
                    dma((2, ZGROUP)), dma((2, ZGROUP)), dma((2, nb)), dma((2, nb)), dma((nlat // 2,)), dma((nlat // 2,)),
                ],
                compiler_params=pltpu.CompilerParams(
                    collective_id=int(dense), has_side_effects=True, vmem_limit_bytes=50000000
                ),
            )(*operands)

        out, flag = run(False)
        out = lax.cond(flag[0] > 0, lambda: run(True)[0], lambda: out)
        return out.reshape(tracers.shape)

    placed = (
        P(None, None, "lat", "lon"),
        P(None, None, "lat", "lon"),
        P(None, None, "lat"),
        P("lat"),
    )
    return jax.shard_map(
        body, mesh=mesh, in_specs=placed, out_specs=P(None, None, "lat", "lon"), check_vma=False
    )
```

```python
import functools

import jax
import jax.numpy as jnp
from jax import lax
from jax.experimental import pallas as pl
from jax.experimental.pallas import tpu as pltpu
from jax.sharding import PartitionSpec as P

LON_TAPS = (-0.0546875, 0.8203125, 0.2734375, -0.0390625)
LAT_TAPS = (-0.0625, 0.5625, 0.5625, -0.0625)
MESH = pl.DeviceIdType.MESH
F32 = jnp.float32
BF16 = jnp.bfloat16
TP = 112
KW = 384
BANDS = 24
ZGROUP = 4
CORES = 2
PITCH = 40
STEP = 4
SLOTS = 512
CAP = 416
REST = 32
FLAG = 120


def tap_select(distance, taps):
    out = jnp.zeros(distance.shape, F32)
    for k in range(4):
        out = jnp.where(distance == k - 1, taps[k], out)
    return out


def lon_matrix(column, lcat, base, lanes=slice(0, 128), edges=True):
    rows = lax.broadcasted_iota(jnp.int32, (128, 128), 0)
    main = tap_select(rows - column, LON_TAPS).astype(BF16)
    lcat[base:base + 128, lanes] = main
    lcat[base + 128:base + 256, lanes] = main
    if edges:
        e = lax.broadcasted_iota(jnp.int32, (16, 128), 0) % 8
        edge = jnp.where(e < 4, e - 4, e + 124)
        lcat[base + 256:base + 272, lanes] = tap_select(edge - column, LON_TAPS).astype(BF16)


def border_cells(o0, o1, direction):
    row = lax.broadcasted_iota(jnp.int32, (8, 128), 0)
    column = lax.broadcasted_iota(jnp.int32, (8, 128), 1) + o0
    reach = lax.rem(row, 4) + o1
    used = jnp.maximum(reach - 1 if direction else 1 - reach, 0)
    inside = jnp.where(column <= 0, 0, jnp.where(column >= 126, 0, 1))
    edge = jnp.where(used > 0, 1.0, 0.0) * jnp.where(inside > 0, 0.0, 1.0)
    used = used * inside
    shared = jnp.zeros((8, 128), F32)
    for k in range(1, 5):
        here = jnp.zeros((8, 128), F32)
        for shift in range(-3, 3):
            hit = jnp.where(o0 == shift, jnp.where(used == k, 1.0, 0.0), 0.0)
            here = jnp.maximum(here, pltpu.roll(hit, shift % 128, 1) if shift else hit)
        for l in range(2):
            top = jnp.max(here[4 * l:4 * l + 4], axis=0, keepdims=True)
            shared = jnp.where(row == 4 * l + k - 1, top, shared)
    i = lax.broadcasted_iota(jnp.int32, (128, 128), 0)
    k = lax.broadcasted_iota(jnp.int32, (128, 128), 1)
    earlier = jnp.where(i < k, 1.0, 0.0).astype(BF16)
    both = jnp.concatenate([shared, edge], axis=0)
    before = jnp.dot(both.astype(BF16), earlier, preferred_element_type=F32)
    own = jnp.broadcast_to(jnp.sum(both, axis=1, keepdims=True), (16, 128))
    inner, outer, count = before[0:8], before[8:16], own[0:8] + own[8:16]
    for n in range(1, 8):
        a = jnp.where(row >= n, pltpu.roll(own[0:8], n, 0), 0.0)
        b = jnp.where(row >= n, pltpu.roll(own[8:16], n, 0), 0.0)
        inner, outer, count = inner + a, outer + b, count + (a + b)
    inner = jnp.where(shared > 0.0, inner, -1.0)
    outer = jnp.where(edge > 0.0, CAP - 1.0 - outer, -1.0)
    return used, inner, outer, count


def places(o0, o1, direction):
    used, inner, outer, count = border_cells(o0, o1, direction)
    row = lax.broadcasted_iota(jnp.int32, (8, 128), 0)
    number = outer
    for k in range(1, 5):
        of_level = jnp.where(row < 4, inner[k - 1:k], inner[k + 3:k + 4])
        for shift in range(-3, 3):
            there = pltpu.roll(of_level, -shift % 128, 1) if shift else of_level
            number = jnp.where(o0 == shift, jnp.where(used == k, there, number), number)
    return number.astype(jnp.int32), count


def kernel(dense, nt, nlat, nlon, x_hbm, off_hbm, target_hbm, mask_hbm, out_ref, flag_hbm,
           xv, xb, offv, target_v, mask_v, es, er, ob, zs, zr, acc, lcat, lpair, sums, flag_v, ra, rb,
           numbers, known, pick, spread, fs, fr,
           local_sem, e_send, e_recv, o_send, o_recv, z_send, z_recv, a_send, a_recv, b_send, b_recv,
           f_send, f_recv):
    lat = lax.axis_index("lat")
    lon = lax.axis_index("lon")
    left = lax.rem(lon + nlon - 1, nlon)
    right = lax.rem(lon + 1, nlon)
    core = lax.rem(lon, CORES)
    zlo = lax.rem(lon // CORES, ZGROUP)
    ny = nlon // (ZGROUP * CORES)
    yy = lon // (ZGROUP * CORES)
    chunks = 8 if dense else SLOTS // 128

    load_x = pltpu.make_async_copy(
        x_hbm, xv.reshape(TP, PITCH, 128).at[pl.ds(0, nt), pl.ds(0, 32), :], local_sem.at[0])
    load_x.start()
    load_off = pltpu.make_async_copy(off_hbm, offv, local_sem.at[1])
    load_off.start()
    load_target = pltpu.make_async_copy(target_hbm, target_v, local_sem.at[2])
    load_target.start()
    load_mask = pltpu.make_async_copy(mask_hbm, mask_v, local_sem.at[3])
    load_mask.start()

    def z_peer(k):
        return {"lon": (yy * ZGROUP + lax.rem(zlo + k, ZGROUP)) * CORES + core}

    def y_peer(k):
        me = yy * CORES + core
        other = lax.rem(me + k, ny * CORES)
        return {"lon": ((other // CORES) * ZGROUP + zlo) * CORES + lax.rem(other, CORES)}

    def x_peer(k):
        return {"lat": lax.rem(lat + 2 * k, nlat)}

    barrier = pltpu.get_barrier_semaphore()

    def greet(device):
        pl.semaphore_signal(barrier, inc=1, device_id=device, device_id_type=MESH)

    has_up = lat > 0
    has_down = lat < nlat - 1

    @pl.when(has_up)
    def _():
        greet({"lat": lat - 1})

    @pl.when(has_down)
    def _():
        greet({"lat": lat + 1})

    for k in range(1, nlat // 2):
        greet(x_peer(k))
    greet({"lon": left})
    greet({"lon": right})
    for k in range(1, ZGROUP):
        greet(z_peer(k))
    for k in range(1, ny * CORES):
        greet(y_peer(k))

    xv[pl.ds(nt * PITCH, (TP - nt) * PITCH), :] = jnp.zeros(((TP - nt) * PITCH, 128), F32)
    for l in range(2):
        for first in (0, 20):
            xb[pl.ds((l * BANDS + first) * TP, 4 * TP), :] = jnp.zeros((4 * TP, KW), BF16)
        lcat[l * KW + 272:(l + 1) * KW, :] = jnp.zeros((112, 128), BF16)
    lpair[272:KW, :] = jnp.zeros((112, 256), BF16)
    lane = lax.broadcasted_iota(jnp.int32, (TP, 128), 1)

    load_off.wait()
    with jax.named_scope("barw"):
        pl.semaphore_wait(
            barrier,
            has_up.astype(jnp.int32) + has_down.astype(jnp.int32) + nlat // 2 + 1 + (ZGROUP - 1) + (ny * CORES - 1))

    ob4 = ob.reshape(2, 2, 2, 4, 128)

    def o_copy(direction):
        return pltpu.make_async_remote_copy(
            src_ref=offv.reshape(2, 2, 16, 128).at[:, :, pl.ds(12 * direction, 4), :],
            dst_ref=ob4.at[direction],
            send_sem=o_send.at[direction], recv_sem=o_recv.at[direction],
            device_id={"lat": lat - 1 + 2 * direction}, device_id_type=MESH)

    @pl.when(has_up)
    def _():
        o_copy(0).start()

    @pl.when(has_down)
    def _():
        o_copy(1).start()

    load_x.wait()

    group = lane // 4

    def pack(step, carry):
        to_left, to_right = carry
        for i in range(STEP):
            lj = step * STEP + i
            v = xv[pl.ds(lj, TP, stride=PITCH), :]
            rolled = pltpu.roll(v, 4 * lj, 1)
            to_left = jnp.where(group == lj, rolled, to_left)
            to_right = jnp.where(group == lax.rem(lj + 31, 32), rolled, to_right)
            hi = v.astype(BF16)
            lo = (v - hi.astype(F32)).astype(BF16)
            row = pl.multiple_of(((lj // 16) * BANDS + 4 + lax.rem(lj, 16)) * TP, 16)
            xb[pl.ds(row, TP), 0:128] = hi
            xb[pl.ds(row, TP), 128:256] = lo
        return to_left, to_right

    zero = jnp.zeros((TP, 128), F32)
    with jax.named_scope("pack"):
        to_left, to_right = lax.fori_loop(0, 32 // STEP, pack, (zero, zero))
    es[0] = to_left
    es[1] = to_right

    def e_copy(side):
        return pltpu.make_async_remote_copy(
            src_ref=es.at[side, pl.ds(0, nt)], dst_ref=er.at[1 - side, pl.ds(0, nt)],
            send_sem=e_send.at[side], recv_sem=e_recv.at[1 - side],
            device_id={"lon": left if side == 0 else right}, device_id_type=MESH)

    def z_copy(direction, s, last=False):
        rows = pl.ds(0, REST if last and not dense else nt)
        return pltpu.make_async_remote_copy(
            src_ref=zs.at[direction, s, rows], dst_ref=zr.at[direction, s, rows],
            send_sem=z_send.at[direction, s], recv_sem=z_recv.at[direction, s],
            device_id={"lat": lat + 1 - 2 * direction}, device_id_type=MESH)

    e_copy(0).start()
    e_copy(1).start()

    f_copies = []
    place = []
    if not dense:
        flag = jnp.zeros((8, 128), F32)
        for direction in range(2):
            o0, o1 = [
                jnp.concatenate([offv[pl.ds(first + 12 * direction, 4), :], offv[pl.ds(first + 16 + 12 * direction, 4), :]], axis=0)
                for first in (0, 32)
            ]
            p, count = places(o0, o1, direction)
            place.append(p)
            exists = has_up if direction == 0 else has_down
            flag = jnp.maximum(flag, jnp.where(count > CAP, exists.astype(F32), 0.0))
        fs[0] = jnp.broadcast_to(jnp.max(flag, axis=(0, 1), keepdims=True), (1, 128))
        for k in range(nlat // 2):
            f_copies.append(pltpu.make_async_remote_copy(
                src_ref=fs.at[min(k, 1)], dst_ref=fr.at[k], send_sem=f_send.at[k], recv_sem=f_recv.at[k],
                device_id=x_peer(k) if k else {"lat": lat + 1 - 2 * lax.rem(lat, 2)}, device_id_type=MESH))
        f_copies[0].start()

    def edges(first, step):
        for i in range(STEP):
            lj = 16 * (step // 2) + first + (4 if first else 12) * lax.rem(step, 2) + i
            shift = lax.rem(132 - 4 * lj, 128)
            a = pltpu.roll(er[0], shift, 1)
            b = pltpu.roll(er[1], shift, 1)
            e = jnp.where(lane < 4, a, b)
            hi = e.astype(BF16).astype(F32)
            both = jnp.where(lane < 8, hi, pltpu.roll(e - hi, 8, 1))
            row = pl.multiple_of(((lj // 16) * BANDS + 4 + lax.rem(lj, 16)) * TP, 16)
            xb[pl.ds(row, TP), 256:384] = both.astype(BF16)
        return 0

    def send_dense(direction):
        def part(s, _):
            l, jj = s // 4, lax.rem(s, 4)
            o0 = ob[pl.ds(16 * direction + s, 1), :]
            o1 = ob[pl.ds(16 * direction + 8 + s, 1), :]
            lon_matrix(o0 + lane[0:1], lcat, 0)
            start = pl.multiple_of((l * BANDS + 4 + 12 * (1 - direction)) * TP, 16)
            y = jnp.dot(xb[pl.ds(start, 4 * TP), :], lcat[0:KW, :], preferred_element_type=F32)
            total = jnp.zeros((TP, 128), F32)
            for hh in range(4):
                w = tap_select(hh + (4 if direction else -4) - jj - o1, LAT_TAPS)
                total = total + w * y[hh * TP:(hh + 1) * TP]
            zs[direction, s] = total
            z_copy(direction, s).start()
            return 0

        lax.fori_loop(0, 8, part, 0)

    def find_cells(direction, edge):
        o0 = ob[pl.ds(16 * direction, 8), :]
        o1 = ob[pl.ds(16 * direction + 8, 8), :]
        row = lax.broadcasted_iota(jnp.int32, (8, 128), 0)
        column = lax.broadcasted_iota(jnp.int32, (8, 128), 1)
        if edge:
            number = numbers[direction, 8:16]
            column = column + o0
            reach = lax.rem(row, 4) + o1
        else:
            _, inner, outer, _ = border_cells(o0, o1, direction)
            number = inner.astype(jnp.int32)
            numbers[direction, 8:16] = outer.astype(jnp.int32)
            reach = 2 + lax.rem(row, 4) if direction else -lax.rem(row, 4)
        number_t = jnp.transpose(jnp.concatenate([number, jnp.zeros((120, 128), jnp.int32)], axis=0))
        first = 256 if edge else 0
        slot = lax.broadcasted_iota(jnp.int32, (128, SLOTS - first), 1) + first
        row16 = lax.broadcasted_iota(jnp.int32, (16, 128), 0)
        cells = []
        for s in range(8):
            pick[s * 128:(s + 1) * 128, first:SLOTS] = jnp.where(number_t[:, s:s + 1] == slot, 1.0, 0.0).astype(BF16)
            v = jnp.where(row16 == 0, column[s:s + 1], jnp.where(row16 == 1, reach[s:s + 1], s // 4))
            cells.append(v.astype(F32).astype(BF16))
        found = jnp.dot(
            jnp.concatenate(cells, axis=1), pick[:, first:SLOTS], preferred_element_type=F32).astype(jnp.int32)
        if edge:
            found = found + known[direction, :, first:SLOTS]
        known[direction, :, first:SLOTS] = found

    def send_packed(direction, c, with_edges):
        here = slice(c * 128, (c + 1) * 128)
        column, reach, level = [known[direction, k:k + 1, here] for k in range(3)]
        depth = KW if with_edges else 256
        y = jnp.zeros((4 * TP, 128), F32)
        for l in range(2):
            lon_matrix(jnp.where(level == l, column, 4096), lcat, l * KW, edges=with_edges)
            start = (l * BANDS + 4 + 12 * (1 - direction)) * TP
            y = y + jnp.dot(
                xb[start:start + 4 * TP, 0:depth], lcat[l * KW:l * KW + depth, :], preferred_element_type=F32)
        total = jnp.zeros((TP, 128), F32)
        for hh in range(4):
            w = tap_select(hh + (4 if direction else -4) - reach, LAT_TAPS)
            total = total + w * y[hh * TP:(hh + 1) * TP]
        last = c == chunks - 1
        if last:
            group = lax.broadcasted_iota(jnp.int32, (REST, 128), 1) // REST
            rest = total[0:REST]
            for n in range(1, 4):
                more = total[n * REST:min((n + 1) * REST, TP)]
                if more.shape[0] < REST:
                    more = jnp.concatenate([more, jnp.zeros((REST - more.shape[0], 128), F32)], axis=0)
                rest = jnp.where(group == n, pltpu.roll(more, n * REST, 1), rest)
            zs[direction, c, 0:REST] = rest
        else:
            zs[direction, c] = total
        z_copy(direction, c, last).start()

    if dense:
        with jax.named_scope("ewait"):
            for side in range(2):
                pltpu.make_async_remote_copy(
                    src_ref=es.at[side, pl.ds(0, nt)], dst_ref=er.at[side, pl.ds(0, nt)], send_sem=e_send.at[side], recv_sem=e_recv.at[side],
                    device_id={"lon": left}, device_id_type=MESH).wait_recv()

        with jax.named_scope("edges"):
            lax.fori_loop(0, 4, lambda step, _: edges(0, step), 0)

    for direction in range(2):
        @pl.when(has_up if direction else has_down)
        def _():
            with jax.named_scope("owait"):
                pltpu.make_async_remote_copy(
                    src_ref=ob4.at[direction], dst_ref=ob4.at[direction],
                    send_sem=o_send.at[direction], recv_sem=o_recv.at[direction],
                    device_id={"lat": lat + 1 - 2 * direction}, device_id_type=MESH).wait_recv()
            with jax.named_scope("part"):
                if dense:
                    send_dense(direction)
                else:
                    find_cells(direction, False)
                    for c in range(2):
                        send_packed(direction, c, False)
                    find_cells(direction, True)

    if not dense:
        with jax.named_scope("ewait"):
            for side in range(2):
                pltpu.make_async_remote_copy(
                    src_ref=es.at[side, pl.ds(0, nt)], dst_ref=er.at[side, pl.ds(0, nt)], send_sem=e_send.at[side], recv_sem=e_recv.at[side],
                    device_id={"lon": left}, device_id_type=MESH).wait_recv()

        with jax.named_scope("edges"):
            lax.fori_loop(0, 4, lambda step, _: edges(0, step), 0)

        for direction in range(2):
            @pl.when(has_up if direction else has_down)
            def _():
                with jax.named_scope("part_edges"):
                    send_packed(direction, 2, True)
                    send_packed(direction, 3, True)

        slot = lax.broadcasted_iota(jnp.int32, (SLOTS, 128), 0)
        with jax.named_scope("spread"):
            for direction in range(2):
                for s in range(8):
                    spread[direction, :, s * 128:(s + 1) * 128] = jnp.where(
                        place[direction][s:s + 1] == slot, 1.0, 0.0).astype(BF16)

        f_copies[0].wait_recv()
        fs[1] = fs[0] + fr[0]
        for c in f_copies[1:]:
            c.start()

    with jax.named_scope("edges2"):
        lax.fori_loop(0, 4, lambda step, _: edges(4, step), 0)

    def own(pair, inner):
        q = lax.rem(pair, 4)
        l, j = pair // 4, 2 * q + (4 if inner else 8 * (q // 2))
        lj = 16 * l + j
        for i in range(2):
            lon_matrix(offv[pl.ds(lj + i, 1), :] + lane[0:1], lpair, 0, slice(128 * i, 128 * i + 128))
        start = pl.multiple_of((l * BANDS + j) * TP, 16)
        y = jnp.dot(xb[pl.ds(start, 10 * TP), :], lpair[...], preferred_element_type=F32)
        for i in range(2):
            o1 = offv[pl.ds(32 + lj + i, 1), :]
            total = jnp.zeros((TP, 128), F32)
            for rr in range(9):
                w = tap_select(rr - 4 - o1, LAT_TAPS)
                total = total + w * y[(rr + i) * TP:(rr + i + 1) * TP, 128 * i:128 * i + 128]
            acc[lj + i] = total
        return 0

    with jax.named_scope("own_inner"):
        lax.fori_loop(0, 8, lambda pair, _: own(pair, True), 0)

    def row_sums(first):
        total = zero
        for n in range(16):
            a = acc[16 * (n // 8) + first + (n % 8 if first else n % 8 + 8 * (n % 8 // 4))]
            total = jnp.where(lane == n, jnp.sum(a * a, axis=1, keepdims=True), total)
        sums[0:TP, :] = total
        sums[TP:128, :] = jnp.zeros((128 - TP, 128), F32)
        return jnp.transpose(sums[...])[0:16]

    def exchange(peer, size, slots, send, recv):
        return [
            pltpu.make_async_remote_copy(
                src_ref=slots.at[0], dst_ref=slots.at[k], send_sem=send.at[k], recv_sem=recv.at[k],
                device_id=peer(k), device_id_type=MESH)
            for k in range(1, size)
        ]

    def total_of(copies, slots):
        total = slots[0]
        for k, c in enumerate(copies):
            c.wait_recv()
            total = total + slots[k + 1]
        return total

    a_copies = [exchange(z_peer, ZGROUP, ra.at[n], a_send.at[n], a_recv.at[n]) for n in range(2)]
    b_copies = [exchange(y_peer, ny * CORES, rb.at[n], b_send.at[n], b_recv.at[n]) for n in range(2)]

    with jax.named_scope("square1"):
        inner = row_sums(4)
    if not dense:
        flag = fs[1]
        for k, c in enumerate(f_copies[1:]):
            c.wait_recv()
            flag = flag + fr[k + 1]
        inner = jnp.where(lax.broadcasted_iota(jnp.int32, (16, 128), 1) >= FLAG, flag, inner)
    ra[0, 0] = inner
    for c in a_copies[0]:
        c.start()

    def save_rows(first):
        for n in range(16):
            lj = 16 * (n // 8) + first + (n % 8 if first else n % 8 + 8 * (n % 8 // 4))
            out_ref[pl.ds(lj, nt, stride=32), :] = acc[lj, 0:nt]

    save_rows(4)

    with jax.named_scope("own_outer"):
        lax.fori_loop(0, 8, lambda pair, _: own(pair, False), 0)

    def add(direction, c, last=False):
        z_copy(direction, c, last).wait_recv()
        if last and not dense:
            rest = zr[direction, c, 0:REST]
            z = jnp.concatenate(
                [rest] + [pltpu.roll(rest, 128 - n * REST, 1)[0:min(REST, TP - n * REST)] for n in range(1, 4)], axis=0)
            z = jnp.where(lane < REST, z, 0.0)
        else:
            z = zr[direction, c]
        if dense:
            lj = (c // 4) * 16 + 12 * direction + lax.rem(c, 4)
            acc[lj] = acc[lj] + z
            return
        hi = z.astype(BF16)
        both = jnp.concatenate([hi, (z - hi.astype(F32)).astype(BF16)], axis=0)
        start = pl.multiple_of(c * 128, 128)
        d = jnp.dot(both, spread[direction, pl.ds(start, 128), :], preferred_element_type=F32)
        for s in range(8):
            lj = (s // 4) * 16 + 12 * direction + s % 4
            acc[lj] = acc[lj] + (d[0:TP, s * 128:(s + 1) * 128] + d[TP:, s * 128:(s + 1) * 128])

    def add_both(c, _, last=False):
        for direction in range(2):
            @pl.when(has_down if direction else has_up)
            def _():
                add(direction, c, last)
        return 0

    with jax.named_scope("add"):
        lax.fori_loop(0, chunks - 1, add_both, 0)
    with jax.named_scope("exA1"):
        rb[0, 0] = total_of(a_copies[0], ra.at[0])
        for c in b_copies[0]:
            c.start()
    with jax.named_scope("add_last"):
        add_both(chunks - 1, 0, True)

    with jax.named_scope("square2"):
        ra[1, 0] = row_sums(0)
    for c in a_copies[1]:
        c.start()
    save_rows(0)
    with jax.named_scope("exA"):
        rb[1, 0] = total_of(a_copies[1], ra.at[1])
    for c in b_copies[1]:
        c.start()
    with jax.named_scope("exB1"):
        inner = total_of(b_copies[0], rb.at[0])
    flag_v[0] = jnp.where(jnp.max(inner[0:8, FLAG:128]) > 0.0, 1, 0)
    put_flag = pltpu.make_async_copy(flag_v, flag_hbm, local_sem.at[0])
    put_flag.start()
    load_target.wait()
    load_mask.wait()
    row = lax.rem(lax.broadcasted_iota(jnp.int32, (32, 128), 0), 16)
    mask = jnp.zeros((32, 128), F32)
    for j in range(16):
        mask = jnp.where(row == j, mask_v[j].astype(F32) * 0.5, mask)
    with jax.named_scope("exB"):
        outer = total_of(b_copies[1], rb.at[1])
    for l in range(2):
        sums[16 * l:16 * l + 4, :] = outer[8 * l:8 * l + 4]
        sums[16 * l + 4:16 * l + 12, :] = inner[8 * l:8 * l + 8]
        sums[16 * l + 12:16 * l + 16, :] = outer[8 * l + 4:8 * l + 8]
    rms = jnp.sqrt(sums[0:32, :] * (1.0 / (128 * nlon)) + 1e-06)
    factor = 1.0 + mask[:, 0:nt] * (target_v[...] / rms[:, 0:nt] - 1.0)
    with jax.named_scope("scale"):
        for t in range(nt):
            here = slice(32 * t, 32 * t + 32)
            out_ref[here, :] = out_ref[here, :] * factor[:, t:t + 1]

    e_copy(0).wait_send()
    e_copy(1).wait_send()
    for c in a_copies[0] + a_copies[1] + b_copies[0] + b_copies[1] + f_copies:
        c.wait_send()
    for direction in range(2):
        @pl.when(has_up if direction else has_down)
        def _():
            o_copy(1 - direction).wait_send()
            lax.fori_loop(0, chunks - 1, lambda s, _: (z_copy(direction, s).wait_send(), 0)[1], 0)
            z_copy(direction, chunks - 1, True).wait_send()
    put_flag.wait()


def solution(mesh):
    nlat, nlon = mesh.shape["lat"], mesh.shape["lon"]

    def body(tracers, offsets, target, band_mask):
        nt = tracers.shape[0]
        nb = nlon // ZGROUP
        vmem, dma = pltpu.VMEM, pltpu.SemaphoreType.DMA
        operands = tuple(pltpu.with_memory_space_constraint(a, pltpu.HBM) for a in (
            tracers.reshape(nt, 32, 128),
            offsets.reshape(64, 128),
            jnp.transpose(target, (1, 2, 0)).reshape(32, nt),
            band_mask,
        ))

        def run(dense):
            return pl.pallas_call(
                functools.partial(kernel, dense, nt, nlat, nlon),
                out_shape=[
                    jax.ShapeDtypeStruct((nt * 32, 128), F32),
                    jax.ShapeDtypeStruct((1,), jnp.int32),
                ],
                in_specs=[pl.BlockSpec(memory_space=pltpu.HBM)] * 4,
                out_specs=[pl.BlockSpec(memory_space=pltpu.VMEM), pl.BlockSpec(memory_space=pltpu.HBM)],
                scratch_shapes=[
                    vmem((TP * PITCH, 128), F32),
                    vmem((2 * BANDS * TP, KW), BF16),
                    vmem((64, 128), jnp.int32),
                    vmem((32, nt), F32),
                    pltpu.SMEM((16,), jnp.int32),
                    vmem((2, TP, 128), F32),
                    vmem((2, TP, 128), F32),
                    vmem((32, 128), jnp.int32),
                    vmem((2, 8, TP, 128), F32),
                    vmem((2, 8, TP, 128), F32),
                    vmem((32, TP, 128), F32),
                    vmem((2 * KW, 128), BF16),
                    vmem((KW, 256), BF16),
                    vmem((128, 128), F32),
                    pltpu.SMEM((1,), jnp.int32),
                    vmem((2, ZGROUP, 16, 128), F32),
                    vmem((2, nb, 16, 128), F32),
                    vmem((2, 16, 128), jnp.int32),
                    vmem((2, 16, SLOTS), jnp.int32),
                    vmem((1024, SLOTS), BF16),
                    vmem((2, SLOTS, 1024), BF16),
                    vmem((2, 1, 128), F32),
                    vmem((nlat // 2, 1, 128), F32),
                    dma((4,)), dma((2,)), dma((2,)), dma((2,)), dma((2,)), dma((2, 8)), dma((2, 8)),
                    dma((2, ZGROUP)), dma((2, ZGROUP)), dma((2, nb)), dma((2, nb)), dma((nlat // 2,)), dma((nlat // 2,)),
                ],
                compiler_params=pltpu.CompilerParams(
                    collective_id=int(dense), has_side_effects=True, vmem_limit_bytes=50000000
                ),
            )(*operands)

        out, flag = run(False)
        out = lax.cond(flag[0] > 0, lambda: run(True)[0], lambda: out)
        return out.reshape(tracers.shape)

    placed = (
        P(None, None, "lat", "lon"),
        P(None, None, "lat", "lon"),
        P(None, None, "lat"),
        P("lat"),
    )
    return jax.shard_map(
        body, mesh=mesh, in_specs=placed, out_specs=P(None, None, "lat", "lon"), check_vma=False
    )
```

```python
import functools

import jax
import jax.numpy as jnp
from jax import lax
from jax.experimental import pallas as pl
from jax.experimental.pallas import tpu as pltpu
from jax.sharding import PartitionSpec as P

LON_TAPS = (-0.0546875, 0.8203125, 0.2734375, -0.0390625)
LAT_TAPS = (-0.0625, 0.5625, 0.5625, -0.0625)
MESH = pl.DeviceIdType.MESH
F32 = jnp.float32
BF16 = jnp.bfloat16
TP = 112
KW = 384
BANDS = 24
ZGROUP = 4
CORES = 2
PITCH = 40
STEP = 4
SLOTS = 512
CAP = 400
REST = 16
FLAG = 120


def tap_select(distance, taps):
    out = jnp.zeros(distance.shape, F32)
    for k in range(4):
        out = jnp.where(distance == k - 1, taps[k], out)
    return out


def lon_matrix(column, lcat, base, lanes=slice(0, 128), edges=True):
    rows = lax.broadcasted_iota(jnp.int32, (128, 128), 0)
    main = tap_select(rows - column, LON_TAPS).astype(BF16)
    lcat[base:base + 128, lanes] = main
    lcat[base + 128:base + 256, lanes] = main
    if edges:
        e = lax.broadcasted_iota(jnp.int32, (16, 128), 0) % 8
        edge = jnp.where(e < 4, e - 4, e + 124)
        lcat[base + 256:base + 272, lanes] = tap_select(edge - column, LON_TAPS).astype(BF16)


def border_cells(o0, o1, direction):
    row = lax.broadcasted_iota(jnp.int32, (8, 128), 0)
    column = lax.broadcasted_iota(jnp.int32, (8, 128), 1) + o0
    reach = lax.rem(row, 4) + o1
    used = jnp.maximum(reach - 1 if direction else 1 - reach, 0)
    inside = jnp.where(column <= 0, 0, jnp.where(column >= 126, 0, 1))
    edge = jnp.where(used > 0, 1.0, 0.0) * jnp.where(inside > 0, 0.0, 1.0)
    used = used * inside
    shared = jnp.zeros((8, 128), F32)
    for k in range(1, 5):
        here = jnp.zeros((8, 128), F32)
        for shift in range(-3, 3):
            hit = jnp.where(o0 == shift, jnp.where(used == k, 1.0, 0.0), 0.0)
            here = jnp.maximum(here, pltpu.roll(hit, shift % 128, 1) if shift else hit)
        for l in range(2):
            top = jnp.max(here[4 * l:4 * l + 4], axis=0, keepdims=True)
            shared = jnp.where(row == 4 * l + k - 1, top, shared)
    i = lax.broadcasted_iota(jnp.int32, (128, 128), 0)
    k = lax.broadcasted_iota(jnp.int32, (128, 128), 1)
    earlier = jnp.where(i < k, 1.0, 0.0).astype(BF16)
    both = jnp.concatenate([shared, edge], axis=0)
    before = jnp.dot(both.astype(BF16), earlier, preferred_element_type=F32)
    own = jnp.broadcast_to(jnp.sum(both, axis=1, keepdims=True), (16, 128))
    inner, outer, count = before[0:8], before[8:16], own[0:8] + own[8:16]
    for n in range(1, 8):
        a = jnp.where(row >= n, pltpu.roll(own[0:8], n, 0), 0.0)
        b = jnp.where(row >= n, pltpu.roll(own[8:16], n, 0), 0.0)
        inner, outer, count = inner + a, outer + b, count + (a + b)
    inner = jnp.where(shared > 0.0, inner, -1.0)
    outer = jnp.where(edge > 0.0, CAP - 1.0 - outer, -1.0)
    return used, inner, outer, count


def places(o0, o1, direction):
    used, inner, outer, count = border_cells(o0, o1, direction)
    row = lax.broadcasted_iota(jnp.int32, (8, 128), 0)
    number = outer
    for k in range(1, 5):
        of_level = jnp.where(row < 4, inner[k - 1:k], inner[k + 3:k + 4])
        for shift in range(-3, 3):
            there = pltpu.roll(of_level, -shift % 128, 1) if shift else of_level
            number = jnp.where(o0 == shift, jnp.where(used == k, there, number), number)
    return number.astype(jnp.int32), count


def kernel(dense, nt, nlat, nlon, x_hbm, off_hbm, target_hbm, mask_hbm, out_ref, flag_hbm,
           xv, xb, offv, target_v, mask_v, es, er, ob, zs, zr, acc, lcat, lpair, sums, flag_v, ra, rb,
           numbers, known, pick, spread, fs, fr,
           local_sem, e_send, e_recv, o_send, o_recv, z_send, z_recv, a_send, a_recv, b_send, b_recv,
           f_send, f_recv):
    lat = lax.axis_index("lat")
    lon = lax.axis_index("lon")
    left = lax.rem(lon + nlon - 1, nlon)
    right = lax.rem(lon + 1, nlon)
    core = lax.rem(lon, CORES)
    zlo = lax.rem(lon // CORES, ZGROUP)
    ny = nlon // (ZGROUP * CORES)
    yy = lon // (ZGROUP * CORES)
    chunks = 8 if dense else SLOTS // 128

    load_x = pltpu.make_async_copy(
        x_hbm, xv.reshape(TP, PITCH, 128).at[pl.ds(0, nt), pl.ds(0, 32), :], local_sem.at[0])
    load_x.start()
    load_off = pltpu.make_async_copy(off_hbm, offv, local_sem.at[1])
    load_off.start()
    load_target = pltpu.make_async_copy(target_hbm, target_v, local_sem.at[2])
    load_target.start()
    load_mask = pltpu.make_async_copy(mask_hbm, mask_v, local_sem.at[3])
    load_mask.start()

    def z_peer(k):
        return {"lon": (yy * ZGROUP + lax.rem(zlo + k, ZGROUP)) * CORES + core}

    def y_peer(k):
        me = yy * CORES + core
        other = lax.rem(me + k, ny * CORES)
        return {"lon": ((other // CORES) * ZGROUP + zlo) * CORES + lax.rem(other, CORES)}

    def x_peer(k):
        return {"lat": lax.rem(lat + 2 * k, nlat)}

    barrier = pltpu.get_barrier_semaphore()

    def greet(device):
        pl.semaphore_signal(barrier, inc=1, device_id=device, device_id_type=MESH)

    has_up = lat > 0
    has_down = lat < nlat - 1

    @pl.when(has_up)
    def _():
        greet({"lat": lat - 1})

    @pl.when(has_down)
    def _():
        greet({"lat": lat + 1})

    for k in range(1, nlat // 2):
        greet(x_peer(k))
    greet({"lon": left})
    greet({"lon": right})
    for k in range(1, ZGROUP):
        greet(z_peer(k))
    for k in range(1, ny * CORES):
        greet(y_peer(k))

    xv[pl.ds(nt * PITCH, (TP - nt) * PITCH), :] = jnp.zeros(((TP - nt) * PITCH, 128), F32)
    for l in range(2):
        for first in (0, 20):
            xb[pl.ds((l * BANDS + first) * TP, 4 * TP), :] = jnp.zeros((4 * TP, KW), BF16)
        lcat[l * KW + 272:(l + 1) * KW, :] = jnp.zeros((112, 128), BF16)
    lpair[272:KW, :] = jnp.zeros((112, 256), BF16)
    lane = lax.broadcasted_iota(jnp.int32, (TP, 128), 1)

    load_off.wait()
    with jax.named_scope("barw"):
        pl.semaphore_wait(
            barrier,
            has_up.astype(jnp.int32) + has_down.astype(jnp.int32) + nlat // 2 + 1 + (ZGROUP - 1) + (ny * CORES - 1))

    ob4 = ob.reshape(2, 2, 2, 4, 128)

    def o_copy(direction):
        return pltpu.make_async_remote_copy(
            src_ref=offv.reshape(2, 2, 16, 128).at[:, :, pl.ds(12 * direction, 4), :],
            dst_ref=ob4.at[direction],
            send_sem=o_send.at[direction], recv_sem=o_recv.at[direction],
            device_id={"lat": lat - 1 + 2 * direction}, device_id_type=MESH)

    @pl.when(has_up)
    def _():
        o_copy(0).start()

    @pl.when(has_down)
    def _():
        o_copy(1).start()

    load_x.wait()

    group = lane // 4

    def pack(step, carry):
        to_left, to_right = carry
        for i in range(STEP):
            lj = step * STEP + i
            v = xv[pl.ds(lj, TP, stride=PITCH), :]
            rolled = pltpu.roll(v, 4 * lj, 1)
            to_left = jnp.where(group == lj, rolled, to_left)
            to_right = jnp.where(group == lax.rem(lj + 31, 32), rolled, to_right)
            hi = v.astype(BF16)
            lo = (v - hi.astype(F32)).astype(BF16)
            row = pl.multiple_of(((lj // 16) * BANDS + 4 + lax.rem(lj, 16)) * TP, 16)
            xb[pl.ds(row, TP), 0:128] = hi
            xb[pl.ds(row, TP), 128:256] = lo
        return to_left, to_right

    zero = jnp.zeros((TP, 128), F32)
    with jax.named_scope("pack"):
        to_left, to_right = lax.fori_loop(0, 32 // STEP, pack, (zero, zero))
    es[0] = to_left
    es[1] = to_right

    def e_copy(side):
        return pltpu.make_async_remote_copy(
            src_ref=es.at[side, pl.ds(0, nt)], dst_ref=er.at[1 - side, pl.ds(0, nt)],
            send_sem=e_send.at[side], recv_sem=e_recv.at[1 - side],
            device_id={"lon": left if side == 0 else right}, device_id_type=MESH)

    def z_copy(direction, s, last=False):
        rows = pl.ds(0, REST if last and not dense else nt)
        return pltpu.make_async_remote_copy(
            src_ref=zs.at[direction, s, rows], dst_ref=zr.at[direction, s, rows],
            send_sem=z_send.at[direction, s], recv_sem=z_recv.at[direction, s],
            device_id={"lat": lat + 1 - 2 * direction}, device_id_type=MESH)

    e_copy(0).start()
    e_copy(1).start()

    f_copies = []
    place = []
    if not dense:
        flag = jnp.zeros((8, 128), F32)
        for direction in range(2):
            o0, o1 = [
                jnp.concatenate([offv[pl.ds(first + 12 * direction, 4), :], offv[pl.ds(first + 16 + 12 * direction, 4), :]], axis=0)
                for first in (0, 32)
            ]
            p, count = places(o0, o1, direction)
            place.append(p)
            exists = has_up if direction == 0 else has_down
            flag = jnp.maximum(flag, jnp.where(count > CAP, exists.astype(F32), 0.0))
        fs[0] = jnp.broadcast_to(jnp.max(flag, axis=(0, 1), keepdims=True), (1, 128))
        for k in range(nlat // 2):
            f_copies.append(pltpu.make_async_remote_copy(
                src_ref=fs.at[min(k, 1)], dst_ref=fr.at[k], send_sem=f_send.at[k], recv_sem=f_recv.at[k],
                device_id=x_peer(k) if k else {"lat": lat + 1 - 2 * lax.rem(lat, 2)}, device_id_type=MESH))
        f_copies[0].start()

        slot = lax.broadcasted_iota(jnp.int32, (SLOTS, 128), 0)
        with jax.named_scope("spread"):
            for direction in range(2):
                for s in range(8):
                    spread[direction, :, s * 128:(s + 1) * 128] = jnp.where(
                        place[direction][s:s + 1] == slot, 1.0, 0.0).astype(BF16)

    def edges(first, step):
        for i in range(STEP):
            lj = 16 * (step // 2) + first + (4 if first else 12) * lax.rem(step, 2) + i
            shift = lax.rem(132 - 4 * lj, 128)
            a = pltpu.roll(er[0], shift, 1)
            b = pltpu.roll(er[1], shift, 1)
            e = jnp.where(lane < 4, a, b)
            hi = e.astype(BF16).astype(F32)
            both = jnp.where(lane < 8, hi, pltpu.roll(e - hi, 8, 1))
            row = pl.multiple_of(((lj // 16) * BANDS + 4 + lax.rem(lj, 16)) * TP, 16)
            xb[pl.ds(row, TP), 256:384] = both.astype(BF16)
        return 0

    def send_dense(direction):
        def part(s, _):
            l, jj = s // 4, lax.rem(s, 4)
            o0 = ob[pl.ds(16 * direction + s, 1), :]
            o1 = ob[pl.ds(16 * direction + 8 + s, 1), :]
            lon_matrix(o0 + lane[0:1], lcat, 0)
            start = pl.multiple_of((l * BANDS + 4 + 12 * (1 - direction)) * TP, 16)
            y = jnp.dot(xb[pl.ds(start, 4 * TP), :], lcat[0:KW, :], preferred_element_type=F32)
            total = jnp.zeros((TP, 128), F32)
            for hh in range(4):
                w = tap_select(hh + (4 if direction else -4) - jj - o1, LAT_TAPS)
                total = total + w * y[hh * TP:(hh + 1) * TP]
            zs[direction, s] = total
            z_copy(direction, s).start()
            return 0

        lax.fori_loop(0, 8, part, 0)

    def find_cells(direction, edge):
        o0 = ob[pl.ds(16 * direction, 8), :]
        o1 = ob[pl.ds(16 * direction + 8, 8), :]
        row = lax.broadcasted_iota(jnp.int32, (8, 128), 0)
        column = lax.broadcasted_iota(jnp.int32, (8, 128), 1)
        if edge:
            number = numbers[direction, 8:16]
            column = column + o0
            reach = lax.rem(row, 4) + o1
        else:
            _, inner, outer, _ = border_cells(o0, o1, direction)
            number = inner.astype(jnp.int32)
            numbers[direction, 8:16] = outer.astype(jnp.int32)
            reach = 2 + lax.rem(row, 4) if direction else -lax.rem(row, 4)
        number_t = jnp.transpose(jnp.concatenate([number, jnp.zeros((120, 128), jnp.int32)], axis=0))
        first = 256 if edge else 0
        slot = lax.broadcasted_iota(jnp.int32, (128, SLOTS - first), 1) + first
        row16 = lax.broadcasted_iota(jnp.int32, (16, 128), 0)
        cells = []
        for s in range(8):
            pick[s * 128:(s + 1) * 128, first:SLOTS] = jnp.where(number_t[:, s:s + 1] == slot, 1.0, 0.0).astype(BF16)
            v = jnp.where(row16 == 0, column[s:s + 1], jnp.where(row16 == 1, reach[s:s + 1], s // 4))
            cells.append(v.astype(F32).astype(BF16))
        found = jnp.dot(
            jnp.concatenate(cells, axis=1), pick[:, first:SLOTS], preferred_element_type=F32).astype(jnp.int32)
        if edge:
            found = found + known[direction, :, first:SLOTS]
        known[direction, :, first:SLOTS] = found

    def send_packed(direction, c, with_edges):
        here = slice(c * 128, (c + 1) * 128)
        column, reach, level = [known[direction, k:k + 1, here] for k in range(3)]
        depth = KW if with_edges else 256
        y = jnp.zeros((4 * TP, 128), F32)
        for l in range(2):
            lon_matrix(jnp.where(level == l, column, 4096), lcat, l * KW, edges=with_edges)
            start = (l * BANDS + 4 + 12 * (1 - direction)) * TP
            y = y + jnp.dot(
                xb[start:start + 4 * TP, 0:depth], lcat[l * KW:l * KW + depth, :], preferred_element_type=F32)
        total = jnp.zeros((TP, 128), F32)
        for hh in range(4):
            w = tap_select(hh + (4 if direction else -4) - reach, LAT_TAPS)
            total = total + w * y[hh * TP:(hh + 1) * TP]
        last = c == chunks - 1
        if last:
            group = lax.broadcasted_iota(jnp.int32, (REST, 128), 1) // REST
            rest = total[0:REST]
            for n in range(1, TP // REST):
                more = total[n * REST:(n + 1) * REST]
                rest = jnp.where(group == n, pltpu.roll(more, n * REST, 1), rest)
            zs[direction, c, 0:REST] = rest
        else:
            zs[direction, c] = total
        z_copy(direction, c, last).start()

    if dense:
        with jax.named_scope("ewait"):
            for side in range(2):
                pltpu.make_async_remote_copy(
                    src_ref=es.at[side, pl.ds(0, nt)], dst_ref=er.at[side, pl.ds(0, nt)], send_sem=e_send.at[side], recv_sem=e_recv.at[side],
                    device_id={"lon": left}, device_id_type=MESH).wait_recv()

        with jax.named_scope("edges"):
            lax.fori_loop(0, 4, lambda step, _: edges(0, step), 0)

    for direction in range(2):
        @pl.when(has_up if direction else has_down)
        def _():
            with jax.named_scope("owait"):
                pltpu.make_async_remote_copy(
                    src_ref=ob4.at[direction], dst_ref=ob4.at[direction],
                    send_sem=o_send.at[direction], recv_sem=o_recv.at[direction],
                    device_id={"lat": lat + 1 - 2 * direction}, device_id_type=MESH).wait_recv()
            with jax.named_scope("part"):
                if dense:
                    send_dense(direction)
                else:
                    find_cells(direction, False)
                    for c in range(2):
                        send_packed(direction, c, False)
                    find_cells(direction, True)

    if not dense:
        with jax.named_scope("ewait"):
            for side in range(2):
                pltpu.make_async_remote_copy(
                    src_ref=es.at[side, pl.ds(0, nt)], dst_ref=er.at[side, pl.ds(0, nt)], send_sem=e_send.at[side], recv_sem=e_recv.at[side],
                    device_id={"lon": left}, device_id_type=MESH).wait_recv()

        with jax.named_scope("edges"):
            lax.fori_loop(0, 4, lambda step, _: edges(0, step), 0)

        for direction in range(2):
            @pl.when(has_up if direction else has_down)
            def _():
                with jax.named_scope("part_edges"):
                    send_packed(direction, 2, True)
                    send_packed(direction, 3, True)

        f_copies[0].wait_recv()
        fs[1] = fs[0] + fr[0]
        for c in f_copies[1:]:
            c.start()

    with jax.named_scope("edges2"):
        lax.fori_loop(0, 4, lambda step, _: edges(4, step), 0)

    def own(pair, inner):
        q = lax.rem(pair, 4)
        l, j = pair // 4, 2 * q + (4 if inner else 8 * (q // 2))
        lj = 16 * l + j
        for i in range(2):
            lon_matrix(offv[pl.ds(lj + i, 1), :] + lane[0:1], lpair, 0, slice(128 * i, 128 * i + 128))
        start = pl.multiple_of((l * BANDS + j) * TP, 16)
        y = jnp.dot(xb[pl.ds(start, 10 * TP), :], lpair[...], preferred_element_type=F32)
        for i in range(2):
            o1 = offv[pl.ds(32 + lj + i, 1), :]
            total = jnp.zeros((TP, 128), F32)
            for rr in range(9):
                w = tap_select(rr - 4 - o1, LAT_TAPS)
                total = total + w * y[(rr + i) * TP:(rr + i + 1) * TP, 128 * i:128 * i + 128]
            acc[lj + i] = total
        return 0

    with jax.named_scope("own_inner"):
        lax.fori_loop(0, 8, lambda pair, _: own(pair, True), 0)

    def row_sums(first):
        total = zero
        for n in range(16):
            a = acc[16 * (n // 8) + first + (n % 8 if first else n % 8 + 8 * (n % 8 // 4))]
            total = jnp.where(lane == n, jnp.sum(a * a, axis=1, keepdims=True), total)
        sums[0:TP, :] = total
        sums[TP:128, :] = jnp.zeros((128 - TP, 128), F32)
        return jnp.transpose(sums[...])[0:16]

    def exchange(peer, size, slots, send, recv):
        return [
            pltpu.make_async_remote_copy(
                src_ref=slots.at[0], dst_ref=slots.at[k], send_sem=send.at[k], recv_sem=recv.at[k],
                device_id=peer(k), device_id_type=MESH)
            for k in range(1, size)
        ]

    def total_of(copies, slots):
        total = slots[0]
        for k, c in enumerate(copies):
            c.wait_recv()
            total = total + slots[k + 1]
        return total

    a_copies = [exchange(z_peer, ZGROUP, ra.at[n], a_send.at[n], a_recv.at[n]) for n in range(2)]
    b_copies = [exchange(y_peer, ny * CORES, rb.at[n], b_send.at[n], b_recv.at[n]) for n in range(2)]

    with jax.named_scope("square1"):
        inner = row_sums(4)
    if not dense:
        flag = fs[1]
        for k, c in enumerate(f_copies[1:]):
            c.wait_recv()
            flag = flag + fr[k + 1]
        inner = jnp.where(lax.broadcasted_iota(jnp.int32, (16, 128), 1) >= FLAG, flag, inner)
    ra[0, 0] = inner
    for c in a_copies[0]:
        c.start()

    def save_rows(first):
        for n in range(16):
            lj = 16 * (n // 8) + first + (n % 8 if first else n % 8 + 8 * (n % 8 // 4))
            out_ref[pl.ds(lj, nt, stride=32), :] = acc[lj, 0:nt]

    with jax.named_scope("own_outer"):
        lax.fori_loop(0, 8, lambda pair, _: own(pair, False), 0)

    def add(direction, c, last=False):
        z_copy(direction, c, last).wait_recv()
        if last and not dense:
            rest = zr[direction, c, 0:REST]
            z = jnp.concatenate([rest] + [pltpu.roll(rest, 128 - n * REST, 1) for n in range(1, TP // REST)], axis=0)
            z = jnp.where(lane < REST, z, 0.0)
        else:
            z = zr[direction, c]
        if dense:
            lj = (c // 4) * 16 + 12 * direction + lax.rem(c, 4)
            acc[lj] = acc[lj] + z
            return
        hi = z.astype(BF16)
        both = jnp.concatenate([hi, (z - hi.astype(F32)).astype(BF16)], axis=0)
        start = pl.multiple_of(c * 128, 128)
        d = jnp.dot(both, spread[direction, pl.ds(start, 128), :], preferred_element_type=F32)
        for s in range(8):
            lj = (s // 4) * 16 + 12 * direction + s % 4
            acc[lj] = acc[lj] + (d[0:TP, s * 128:(s + 1) * 128] + d[TP:, s * 128:(s + 1) * 128])

    def add_both(c, _, last=False):
        for direction in range(2):
            @pl.when(has_down if direction else has_up)
            def _():
                add(direction, c, last)
        return 0

    with jax.named_scope("add"):
        lax.fori_loop(0, chunks - 1, add_both, 0)
    with jax.named_scope("exA1"):
        rb[0, 0] = total_of(a_copies[0], ra.at[0])
        for c in b_copies[0]:
            c.start()
    with jax.named_scope("add_last"):
        add_both(chunks - 1, 0, True)

    with jax.named_scope("square2"):
        ra[1, 0] = row_sums(0)
    for c in a_copies[1]:
        c.start()
    save_rows(4)
    save_rows(0)
    with jax.named_scope("exA"):
        rb[1, 0] = total_of(a_copies[1], ra.at[1])
    for c in b_copies[1]:
        c.start()
    with jax.named_scope("exB1"):
        inner = total_of(b_copies[0], rb.at[0])
    flag_v[0] = jnp.where(jnp.max(inner[0:8, FLAG:128]) > 0.0, 1, 0)
    put_flag = pltpu.make_async_copy(flag_v, flag_hbm, local_sem.at[0])
    put_flag.start()
    load_target.wait()
    load_mask.wait()
    row = lax.rem(lax.broadcasted_iota(jnp.int32, (32, 128), 0), 16)
    mask = jnp.zeros((32, 128), F32)
    for j in range(16):
        mask = jnp.where(row == j, mask_v[j].astype(F32) * 0.5, mask)
    with jax.named_scope("exB"):
        outer = total_of(b_copies[1], rb.at[1])
    for l in range(2):
        sums[16 * l:16 * l + 4, :] = outer[8 * l:8 * l + 4]
        sums[16 * l + 4:16 * l + 12, :] = inner[8 * l:8 * l + 8]
        sums[16 * l + 12:16 * l + 16, :] = outer[8 * l + 4:8 * l + 8]
    rms = jnp.sqrt(sums[0:32, :] * (1.0 / (128 * nlon)) + 1e-06)
    factor = 1.0 + mask[:, 0:nt] * (target_v[...] / rms[:, 0:nt] - 1.0)
    with jax.named_scope("scale"):
        for t in range(nt):
            here = slice(32 * t, 32 * t + 32)
            out_ref[here, :] = out_ref[here, :] * factor[:, t:t + 1]

    e_copy(0).wait_send()
    e_copy(1).wait_send()
    for c in a_copies[0] + a_copies[1] + b_copies[0] + b_copies[1] + f_copies:
        c.wait_send()
    for direction in range(2):
        @pl.when(has_up if direction else has_down)
        def _():
            o_copy(1 - direction).wait_send()
            lax.fori_loop(0, chunks - 1, lambda s, _: (z_copy(direction, s).wait_send(), 0)[1], 0)
            z_copy(direction, chunks - 1, True).wait_send()
    put_flag.wait()


def solution(mesh):
    nlat, nlon = mesh.shape["lat"], mesh.shape["lon"]

    def body(tracers, offsets, target, band_mask):
        nt = tracers.shape[0]
        nb = nlon // ZGROUP
        vmem, dma = pltpu.VMEM, pltpu.SemaphoreType.DMA
        operands = tuple(pltpu.with_memory_space_constraint(a, pltpu.HBM) for a in (
            tracers.reshape(nt, 32, 128),
            offsets.reshape(64, 128),
            jnp.transpose(target, (1, 2, 0)).reshape(32, nt),
            band_mask,
        ))

        def run(dense):
            return pl.pallas_call(
                functools.partial(kernel, dense, nt, nlat, nlon),
                out_shape=[
                    jax.ShapeDtypeStruct((nt * 32, 128), F32),
                    jax.ShapeDtypeStruct((1,), jnp.int32),
                ],
                in_specs=[pl.BlockSpec(memory_space=pltpu.HBM)] * 4,
                out_specs=[pl.BlockSpec(memory_space=pltpu.VMEM), pl.BlockSpec(memory_space=pltpu.HBM)],
                scratch_shapes=[
                    vmem((TP * PITCH, 128), F32),
                    vmem((2 * BANDS * TP, KW), BF16),
                    vmem((64, 128), jnp.int32),
                    vmem((32, nt), F32),
                    pltpu.SMEM((16,), jnp.int32),
                    vmem((2, TP, 128), F32),
                    vmem((2, TP, 128), F32),
                    vmem((32, 128), jnp.int32),
                    vmem((2, 8, TP, 128), F32),
                    vmem((2, 8, TP, 128), F32),
                    vmem((32, TP, 128), F32),
                    vmem((2 * KW, 128), BF16),
                    vmem((KW, 256), BF16),
                    vmem((128, 128), F32),
                    pltpu.SMEM((1,), jnp.int32),
                    vmem((2, ZGROUP, 16, 128), F32),
                    vmem((2, nb, 16, 128), F32),
                    vmem((2, 16, 128), jnp.int32),
                    vmem((2, 16, SLOTS), jnp.int32),
                    vmem((1024, SLOTS), BF16),
                    vmem((2, SLOTS, 1024), BF16),
                    vmem((2, 1, 128), F32),
                    vmem((nlat // 2, 1, 128), F32),
                    dma((4,)), dma((2,)), dma((2,)), dma((2,)), dma((2,)), dma((2, 8)), dma((2, 8)),
                    dma((2, ZGROUP)), dma((2, ZGROUP)), dma((2, nb)), dma((2, nb)), dma((nlat // 2,)), dma((nlat // 2,)),
                ],
                compiler_params=pltpu.CompilerParams(
                    collective_id=int(dense), has_side_effects=True, vmem_limit_bytes=50000000
                ),
            )(*operands)

        out, flag = run(False)
        out = lax.cond(flag[0] > 0, lambda: run(True)[0], lambda: out)
        return out.reshape(tracers.shape)

    placed = (
        P(None, None, "lat", "lon"),
        P(None, None, "lat", "lon"),
        P(None, None, "lat"),
        P("lat"),
    )
    return jax.shard_map(
        body, mesh=mesh, in_specs=placed, out_specs=P(None, None, "lat", "lon"), check_vma=False
    )
```

```python
import functools

import jax
import jax.numpy as jnp
from jax import lax
from jax.experimental import pallas as pl
from jax.experimental.pallas import tpu as pltpu
from jax.sharding import PartitionSpec as P

LON_TAPS = (-0.0546875, 0.8203125, 0.2734375, -0.0390625)
LAT_TAPS = (-0.0625, 0.5625, 0.5625, -0.0625)
MESH = pl.DeviceIdType.MESH
F32 = jnp.float32
BF16 = jnp.bfloat16
TP = 112
KW = 384
BANDS = 24
ZGROUP = 4
CORES = 2
PITCH = 40
STEP = 4
SLOTS = 512
CAP = 400
REST = 16
FLAG = 120


def tap_select(distance, taps):
    out = jnp.zeros(distance.shape, F32)
    for k in range(4):
        out = jnp.where(distance == k - 1, taps[k], out)
    return out


def lon_matrix(column, lcat, base, lanes=slice(0, 128), edges=True):
    rows = lax.broadcasted_iota(jnp.int32, (128, 128), 0)
    main = tap_select(rows - column, LON_TAPS).astype(BF16)
    lcat[base:base + 128, lanes] = main
    lcat[base + 128:base + 256, lanes] = main
    if edges:
        e = lax.broadcasted_iota(jnp.int32, (16, 128), 0) % 8
        edge = jnp.where(e < 4, e - 4, e + 124)
        lcat[base + 256:base + 272, lanes] = tap_select(edge - column, LON_TAPS).astype(BF16)


def border_cells(o0, o1, direction):
    row = lax.broadcasted_iota(jnp.int32, (8, 128), 0)
    column = lax.broadcasted_iota(jnp.int32, (8, 128), 1) + o0
    reach = lax.rem(row, 4) + o1
    used = jnp.maximum(reach - 1 if direction else 1 - reach, 0)
    inside = jnp.where(column <= 0, 0, jnp.where(column >= 126, 0, 1))
    edge = jnp.where(used > 0, 1.0, 0.0) * jnp.where(inside > 0, 0.0, 1.0)
    used = used * inside
    shared = jnp.zeros((8, 128), F32)
    for k in range(1, 5):
        here = jnp.zeros((8, 128), F32)
        for shift in range(-3, 3):
            hit = jnp.where(o0 == shift, jnp.where(used == k, 1.0, 0.0), 0.0)
            here = jnp.maximum(here, pltpu.roll(hit, shift % 128, 1) if shift else hit)
        for l in range(2):
            top = jnp.max(here[4 * l:4 * l + 4], axis=0, keepdims=True)
            shared = jnp.where(row == 4 * l + k - 1, top, shared)
    i = lax.broadcasted_iota(jnp.int32, (128, 128), 0)
    k = lax.broadcasted_iota(jnp.int32, (128, 128), 1)
    earlier = jnp.where(i < k, 1.0, 0.0).astype(BF16)
    both = jnp.concatenate([shared, edge], axis=0)
    before = jnp.dot(both.astype(BF16), earlier, preferred_element_type=F32)
    own = jnp.broadcast_to(jnp.sum(both, axis=1, keepdims=True), (16, 128))
    inner, outer, count = before[0:8], before[8:16], own[0:8] + own[8:16]
    for n in range(1, 8):
        a = jnp.where(row >= n, pltpu.roll(own[0:8], n, 0), 0.0)
        b = jnp.where(row >= n, pltpu.roll(own[8:16], n, 0), 0.0)
        inner, outer, count = inner + a, outer + b, count + (a + b)
    inner = jnp.where(shared > 0.0, inner, -1.0)
    outer = jnp.where(edge > 0.0, CAP - 1.0 - outer, -1.0)
    return used, inner, outer, count


def places(o0, o1, direction):
    used, inner, outer, count = border_cells(o0, o1, direction)
    row = lax.broadcasted_iota(jnp.int32, (8, 128), 0)
    number = outer
    for k in range(1, 5):
        of_level = jnp.where(row < 4, inner[k - 1:k], inner[k + 3:k + 4])
        for shift in range(-3, 3):
            there = pltpu.roll(of_level, -shift % 128, 1) if shift else of_level
            number = jnp.where(o0 == shift, jnp.where(used == k, there, number), number)
    return number.astype(jnp.int32), count


def kernel(dense, nt, nlat, nlon, x_hbm, off_hbm, target_hbm, mask_hbm, out_ref, flag_hbm,
           xv, xb, offv, target_v, mask_v, es, er, ob, zs, zr, acc, lcat, lpair, sums, flag_v, ra, rb,
           numbers, known, pick, spread, fs, fr,
           local_sem, e_send, e_recv, o_send, o_recv, z_send, z_recv, a_send, a_recv, b_send, b_recv,
           f_send, f_recv):
    lat = lax.axis_index("lat")
    lon = lax.axis_index("lon")
    left = lax.rem(lon + nlon - 1, nlon)
    right = lax.rem(lon + 1, nlon)
    core = lax.rem(lon, CORES)
    zlo = lax.rem(lon // CORES, ZGROUP)
    ny = nlon // (ZGROUP * CORES)
    yy = lon // (ZGROUP * CORES)
    chunks = 8 if dense else SLOTS // 128

    load_x = pltpu.make_async_copy(
        x_hbm, xv.reshape(TP, PITCH, 128).at[pl.ds(0, nt), pl.ds(0, 32), :], local_sem.at[0])
    load_x.start()
    load_off = pltpu.make_async_copy(off_hbm, offv.at[pl.ds(0, 64)], local_sem.at[1])
    load_off.start()
    load_target = pltpu.make_async_copy(target_hbm, target_v, local_sem.at[2])
    load_target.start()
    load_mask = pltpu.make_async_copy(mask_hbm, mask_v, local_sem.at[3])
    load_mask.start()

    def z_peer(k):
        return {"lon": (yy * ZGROUP + lax.rem(zlo + k, ZGROUP)) * CORES + core}

    def y_peer(k):
        me = yy * CORES + core
        other = lax.rem(me + k, ny * CORES)
        return {"lon": ((other // CORES) * ZGROUP + zlo) * CORES + lax.rem(other, CORES)}

    def x_peer(k):
        return {"lat": lax.rem(lat + 2 * k, nlat)}

    barrier = pltpu.get_barrier_semaphore()

    def greet(device):
        pl.semaphore_signal(barrier, inc=1, device_id=device, device_id_type=MESH)

    has_up = lat > 0
    has_down = lat < nlat - 1

    @pl.when(has_up)
    def _():
        greet({"lat": lat - 1})

    @pl.when(has_down)
    def _():
        greet({"lat": lat + 1})

    for k in range(1, nlat // 2):
        greet(x_peer(k))
    greet({"lon": left})
    greet({"lon": right})
    for k in range(1, ZGROUP):
        greet(z_peer(k))
    for k in range(1, ny * CORES):
        greet(y_peer(k))

    xv[pl.ds(nt * PITCH, (TP - nt) * PITCH), :] = jnp.zeros(((TP - nt) * PITCH, 128), F32)
    for l in range(2):
        for first in (0, 20):
            xb[pl.ds((l * BANDS + first) * TP, 4 * TP), :] = jnp.zeros((4 * TP, KW), BF16)
        lcat[l * KW + 272:(l + 1) * KW, :] = jnp.zeros((112, 128), BF16)
    lpair[272:KW, :] = jnp.zeros((112, 256), BF16)
    lane = lax.broadcasted_iota(jnp.int32, (TP, 128), 1)

    load_off.wait()
    with jax.named_scope("barw"):
        pl.semaphore_wait(
            barrier,
            has_up.astype(jnp.int32) + has_down.astype(jnp.int32) + nlat // 2 + 1 + (ZGROUP - 1) + (ny * CORES - 1))

    ob4 = ob.at[pl.ds(0, 32)].reshape(2, 2, 2, 4, 128)

    def o_copy(direction):
        return pltpu.make_async_remote_copy(
            src_ref=offv.at[pl.ds(0, 64)].reshape(2, 2, 16, 128).at[:, :, pl.ds(12 * direction, 4), :],
            dst_ref=ob4.at[direction],
            send_sem=o_send.at[direction], recv_sem=o_recv.at[direction],
            device_id={"lat": lat - 1 + 2 * direction}, device_id_type=MESH)

    @pl.when(has_up)
    def _():
        o_copy(0).start()

    @pl.when(has_down)
    def _():
        o_copy(1).start()

    load_x.wait()

    group = lane // 4

    def pack(step, carry):
        to_left, to_right = carry
        for i in range(STEP):
            lj = step * STEP + i
            v = xv[pl.ds(lj, TP, stride=PITCH), :]
            rolled = pltpu.roll(v, 4 * lj, 1)
            to_left = jnp.where(group == lj, rolled, to_left)
            to_right = jnp.where(group == lax.rem(lj + 31, 32), rolled, to_right)
            hi = v.astype(BF16)
            lo = (v - hi.astype(F32)).astype(BF16)
            row = pl.multiple_of(((lj // 16) * BANDS + 4 + lax.rem(lj, 16)) * TP, 16)
            xb[pl.ds(row, TP), 0:128] = hi
            xb[pl.ds(row, TP), 128:256] = lo
        return to_left, to_right

    zero = jnp.zeros((TP, 128), F32)
    with jax.named_scope("pack"):
        to_left, to_right = lax.fori_loop(0, 32 // STEP, pack, (zero, zero))
    es[0] = to_left
    es[1] = to_right

    def e_copy(side):
        return pltpu.make_async_remote_copy(
            src_ref=es.at[side, pl.ds(0, nt)], dst_ref=er.at[1 - side, pl.ds(0, nt)],
            send_sem=e_send.at[side], recv_sem=e_recv.at[1 - side],
            device_id={"lon": left if side == 0 else right}, device_id_type=MESH)

    def z_copy(direction, s, last=False):
        rows = pl.ds(0, REST if last and not dense else nt)
        return pltpu.make_async_remote_copy(
            src_ref=zs.at[direction, s, rows], dst_ref=zr.at[direction, s, rows],
            send_sem=z_send.at[direction, s], recv_sem=z_recv.at[direction, s],
            device_id={"lat": lat + 1 - 2 * direction}, device_id_type=MESH)

    e_copy(0).start()
    e_copy(1).start()

    f_copies = []
    place = []
    if not dense:
        flag = jnp.zeros((8, 128), F32)
        for direction in range(2):
            o0, o1 = [
                jnp.concatenate([offv[pl.ds(first + 12 * direction, 4), :], offv[pl.ds(first + 16 + 12 * direction, 4), :]], axis=0)
                for first in (0, 32)
            ]
            p, count = places(o0, o1, direction)
            place.append(p)
            exists = has_up if direction == 0 else has_down
            flag = jnp.maximum(flag, jnp.where(count > CAP, exists.astype(F32), 0.0))
        fs[0] = jnp.broadcast_to(jnp.max(flag, axis=(0, 1), keepdims=True), (1, 128))
        for k in range(nlat // 2):
            f_copies.append(pltpu.make_async_remote_copy(
                src_ref=fs.at[min(k, 1)], dst_ref=fr.at[k], send_sem=f_send.at[k], recv_sem=f_recv.at[k],
                device_id=x_peer(k) if k else {"lat": lat + 1 - 2 * lax.rem(lat, 2)}, device_id_type=MESH))
        f_copies[0].start()

        slot = lax.broadcasted_iota(jnp.int32, (SLOTS, 128), 0)
        with jax.named_scope("spread"):
            for direction in range(2):
                for s in range(8):
                    spread[direction, :, s * 128:(s + 1) * 128] = jnp.where(
                        place[direction][s:s + 1] == slot, 1.0, 0.0).astype(BF16)

    def edges(first, step):
        for i in range(STEP):
            lj = 16 * (step // 2) + first + (4 if first else 12) * lax.rem(step, 2) + i
            shift = lax.rem(132 - 4 * lj, 128)
            a = pltpu.roll(er[0], shift, 1)
            b = pltpu.roll(er[1], shift, 1)
            e = jnp.where(lane < 4, a, b)
            hi = e.astype(BF16).astype(F32)
            both = jnp.where(lane < 8, hi, pltpu.roll(e - hi, 8, 1))
            row = pl.multiple_of(((lj // 16) * BANDS + 4 + lax.rem(lj, 16)) * TP, 16)
            xb[pl.ds(row, TP), 256:384] = both.astype(BF16)
        return 0

    def send_dense(direction):
        def part(s, _):
            l, jj = s // 4, lax.rem(s, 4)
            o0 = ob[pl.ds(16 * direction + s, 1), :]
            o1 = ob[pl.ds(16 * direction + 8 + s, 1), :]
            lon_matrix(o0 + lane[0:1], lcat, 0)
            start = pl.multiple_of((l * BANDS + 4 + 12 * (1 - direction)) * TP, 16)
            y = jnp.dot(xb[pl.ds(start, 4 * TP), :], lcat[0:KW, :], preferred_element_type=F32)
            total = jnp.zeros((TP, 128), F32)
            for hh in range(4):
                w = tap_select(hh + (4 if direction else -4) - jj - o1, LAT_TAPS)
                total = total + w * y[hh * TP:(hh + 1) * TP]
            zs[direction, s] = total
            z_copy(direction, s).start()
            return 0

        lax.fori_loop(0, 8, part, 0)

    def find_cells(direction, edge):
        o0 = ob[pl.ds(16 * direction, 8), :]
        o1 = ob[pl.ds(16 * direction + 8, 8), :]
        row = lax.broadcasted_iota(jnp.int32, (8, 128), 0)
        column = lax.broadcasted_iota(jnp.int32, (8, 128), 1)
        if edge:
            number = numbers[direction, 8:16]
            column = column + o0
            reach = lax.rem(row, 4) + o1
        else:
            _, inner, outer, _ = border_cells(o0, o1, direction)
            number = inner.astype(jnp.int32)
            numbers[direction, 8:16] = outer.astype(jnp.int32)
            reach = 2 + lax.rem(row, 4) if direction else -lax.rem(row, 4)
        number_t = jnp.transpose(jnp.concatenate([number, jnp.zeros((120, 128), jnp.int32)], axis=0))
        first = 256 if edge else 0
        slot = lax.broadcasted_iota(jnp.int32, (128, SLOTS - first), 1) + first
        row16 = lax.broadcasted_iota(jnp.int32, (16, 128), 0)
        cells = []
        for s in range(8):
            pick[s * 128:(s + 1) * 128, first:SLOTS] = jnp.where(number_t[:, s:s + 1] == slot, 1.0, 0.0).astype(BF16)
            v = jnp.where(row16 == 0, column[s:s + 1], jnp.where(row16 == 1, reach[s:s + 1], s // 4))
            cells.append(v.astype(F32).astype(BF16))
        found = jnp.dot(
            jnp.concatenate(cells, axis=1), pick[:, first:SLOTS], preferred_element_type=F32).astype(jnp.int32)
        if edge:
            found = found + known[direction, :, first:SLOTS]
        known[direction, :, first:SLOTS] = found

    def send_packed(direction, c, with_edges):
        here = slice(c * 128, (c + 1) * 128)
        column, reach, level = [known[direction, k:k + 1, here] for k in range(3)]
        depth = KW if with_edges else 256
        y = jnp.zeros((4 * TP, 128), F32)
        for l in range(2):
            lon_matrix(jnp.where(level == l, column, 4096), lcat, l * KW, edges=with_edges)
            start = (l * BANDS + 4 + 12 * (1 - direction)) * TP
            y = y + jnp.dot(
                xb[start:start + 4 * TP, 0:depth], lcat[l * KW:l * KW + depth, :], preferred_element_type=F32)
        total = jnp.zeros((TP, 128), F32)
        for hh in range(4):
            w = tap_select(hh + (4 if direction else -4) - reach, LAT_TAPS)
            total = total + w * y[hh * TP:(hh + 1) * TP]
        last = c == chunks - 1
        if last:
            group = lax.broadcasted_iota(jnp.int32, (REST, 128), 1) // REST
            rest = total[0:REST]
            for n in range(1, TP // REST):
                more = total[n * REST:(n + 1) * REST]
                rest = jnp.where(group == n, pltpu.roll(more, n * REST, 1), rest)
            zs[direction, c, 0:REST] = rest
        else:
            zs[direction, c] = total
        z_copy(direction, c, last).start()

    if dense:
        with jax.named_scope("ewait"):
            for side in range(2):
                pltpu.make_async_remote_copy(
                    src_ref=es.at[side, pl.ds(0, nt)], dst_ref=er.at[side, pl.ds(0, nt)], send_sem=e_send.at[side], recv_sem=e_recv.at[side],
                    device_id={"lon": left}, device_id_type=MESH).wait_recv()

        with jax.named_scope("edges"):
            lax.fori_loop(0, 4, lambda step, _: edges(0, step), 0)

    for direction in range(2):
        @pl.when(has_up if direction else has_down)
        def _():
            with jax.named_scope("owait"):
                pltpu.make_async_remote_copy(
                    src_ref=ob4.at[direction], dst_ref=ob4.at[direction],
                    send_sem=o_send.at[direction], recv_sem=o_recv.at[direction],
                    device_id={"lat": lat + 1 - 2 * direction}, device_id_type=MESH).wait_recv()
            with jax.named_scope("part"):
                if dense:
                    send_dense(direction)
                else:
                    find_cells(direction, False)
                    for c in range(2):
                        send_packed(direction, c, False)
                    find_cells(direction, True)

    if not dense:
        with jax.named_scope("ewait"):
            for side in range(2):
                pltpu.make_async_remote_copy(
                    src_ref=es.at[side, pl.ds(0, nt)], dst_ref=er.at[side, pl.ds(0, nt)], send_sem=e_send.at[side], recv_sem=e_recv.at[side],
                    device_id={"lon": left}, device_id_type=MESH).wait_recv()

        with jax.named_scope("edges"):
            lax.fori_loop(0, 4, lambda step, _: edges(0, step), 0)

        for direction in range(2):
            @pl.when(has_up if direction else has_down)
            def _():
                with jax.named_scope("part_edges"):
                    send_packed(direction, 2, True)
                    send_packed(direction, 3, True)

        f_copies[0].wait_recv()
        fs[1] = fs[0] + fr[0]
        for c in f_copies[1:]:
            c.start()

    with jax.named_scope("edges2"):
        lax.fori_loop(0, 4, lambda step, _: edges(4, step), 0)

    def own(pair, inner):
        q = lax.rem(pair, 4)
        l, j = pair // 4, 2 * q + (4 if inner else 8 * (q // 2))
        lj = 16 * l + j
        for i in range(2):
            lon_matrix(offv[pl.ds(lj + i, 1), :] + lane[0:1], lpair, 0, slice(128 * i, 128 * i + 128))
        start = pl.multiple_of((l * BANDS + j) * TP, 16)
        y = jnp.dot(xb[pl.ds(start, 10 * TP), :], lpair[...], preferred_element_type=F32)
        for i in range(2):
            o1 = offv[pl.ds(32 + lj + i, 1), :]
            total = jnp.zeros((TP, 128), F32)
            for rr in range(9):
                w = tap_select(rr - 4 - o1, LAT_TAPS)
                total = total + w * y[(rr + i) * TP:(rr + i + 1) * TP, 128 * i:128 * i + 128]
            acc[lj + i] = total
        return 0

    with jax.named_scope("own_inner"):
        lax.fori_loop(0, 8, lambda pair, _: own(pair, True), 0)

    def row_sums(first):
        total = zero
        for n in range(16):
            a = acc[16 * (n // 8) + first + (n % 8 if first else n % 8 + 8 * (n % 8 // 4))]
            total = jnp.where(lane == n, jnp.sum(a * a, axis=1, keepdims=True), total)
        sums[0:TP, :] = total
        sums[TP:128, :] = jnp.zeros((128 - TP, 128), F32)
        return jnp.transpose(sums[...])[0:16]

    def exchange(peer, size, slots, send, recv):
        return [
            pltpu.make_async_remote_copy(
                src_ref=slots.at[0], dst_ref=slots.at[k], send_sem=send.at[k], recv_sem=recv.at[k],
                device_id=peer(k), device_id_type=MESH)
            for k in range(1, size)
        ]

    def total_of(copies, slots):
        total = slots[0]
        for k, c in enumerate(copies):
            c.wait_recv()
            total = total + slots[k + 1]
        return total

    a_copies = [exchange(z_peer, ZGROUP, ra.at[n], a_send.at[n], a_recv.at[n]) for n in range(2)]
    b_copies = [exchange(y_peer, ny * CORES, rb.at[n], b_send.at[n], b_recv.at[n]) for n in range(2)]

    with jax.named_scope("square1"):
        inner = row_sums(4)
    if not dense:
        flag = fs[1]
        for k, c in enumerate(f_copies[1:]):
            c.wait_recv()
            flag = flag + fr[k + 1]
        inner = jnp.where(lax.broadcasted_iota(jnp.int32, (16, 128), 1) >= FLAG, flag, inner)
    ra[0, 0] = inner
    for c in a_copies[0]:
        c.start()

    def save_rows(first):
        for n in range(16):
            lj = 16 * (n // 8) + first + (n % 8 if first else n % 8 + 8 * (n % 8 // 4))
            out_ref[pl.ds(lj, TP, stride=32), :] = acc[lj]

    with jax.named_scope("own_outer"):
        lax.fori_loop(0, 8, lambda pair, _: own(pair, False), 0)

    def add(direction, c, last=False):
        z_copy(direction, c, last).wait_recv()
        if last and not dense:
            rest = zr[direction, c, 0:REST]
            z = jnp.concatenate([rest] + [pltpu.roll(rest, 128 - n * REST, 1) for n in range(1, TP // REST)], axis=0)
            z = jnp.where(lane < REST, z, 0.0)
        else:
            z = zr[direction, c]
        if dense:
            lj = (c // 4) * 16 + 12 * direction + lax.rem(c, 4)
            acc[lj] = acc[lj] + z
            return
        hi = z.astype(BF16)
        both = jnp.concatenate([hi, (z - hi.astype(F32)).astype(BF16)], axis=0)
        start = pl.multiple_of(c * 128, 128)
        d = jnp.dot(both, spread[direction, pl.ds(start, 128), :], preferred_element_type=F32)
        for s in range(8):
            lj = (s // 4) * 16 + 12 * direction + s % 4
            acc[lj] = acc[lj] + (d[0:TP, s * 128:(s + 1) * 128] + d[TP:, s * 128:(s + 1) * 128])

    def add_both(c, _, last=False):
        for direction in range(2):
            @pl.when(has_down if direction else has_up)
            def _():
                add(direction, c, last)
        return 0

    with jax.named_scope("add"):
        lax.fori_loop(0, chunks - 1, add_both, 0)
    with jax.named_scope("exA1"):
        rb[0, 0] = total_of(a_copies[0], ra.at[0])
        for c in b_copies[0]:
            c.start()
    with jax.named_scope("add_last"):
        add_both(chunks - 1, 0, True)

    with jax.named_scope("square2"):
        ra[1, 0] = row_sums(0)
    for c in a_copies[1]:
        c.start()
    save_rows(4)
    save_rows(0)
    with jax.named_scope("exA"):
        rb[1, 0] = total_of(a_copies[1], ra.at[1])
    for c in b_copies[1]:
        c.start()
    with jax.named_scope("exB1"):
        inner = total_of(b_copies[0], rb.at[0])
    flag_v[0] = jnp.where(jnp.max(inner[0:8, FLAG:128]) > 0.0, 1, 0)
    put_flag = pltpu.make_async_copy(flag_v, flag_hbm, local_sem.at[0])
    put_flag.start()
    load_target.wait()
    load_mask.wait()
    row = lax.rem(lax.broadcasted_iota(jnp.int32, (32, 128), 0), 16)
    mask = jnp.zeros((32, 128), F32)
    for j in range(16):
        mask = jnp.where(row == j, mask_v[j].astype(F32) * 0.5, mask)
    with jax.named_scope("exB"):
        outer = total_of(b_copies[1], rb.at[1])
    for l in range(2):
        sums[16 * l:16 * l + 4, :] = outer[8 * l:8 * l + 4]
        sums[16 * l + 4:16 * l + 12, :] = inner[8 * l:8 * l + 8]
        sums[16 * l + 12:16 * l + 16, :] = outer[8 * l + 4:8 * l + 8]
    rms = jnp.sqrt(sums[0:32, :] * (1.0 / (128 * nlon)) + 1e-06)
    factor = 1.0 + mask[:, 0:nt] * (target_v[...] / rms[:, 0:nt] - 1.0)
    with jax.named_scope("scale"):
        for t in range(nt):
            here = slice(32 * t, 32 * t + 32)
            out_ref[here, :] = out_ref[here, :] * factor[:, t:t + 1]

    e_copy(0).wait_send()
    e_copy(1).wait_send()
    for c in a_copies[0] + a_copies[1] + b_copies[0] + b_copies[1] + f_copies:
        c.wait_send()
    for direction in range(2):
        @pl.when(has_up if direction else has_down)
        def _():
            o_copy(1 - direction).wait_send()
            lax.fori_loop(0, chunks - 1, lambda s, _: (z_copy(direction, s).wait_send(), 0)[1], 0)
            z_copy(direction, chunks - 1, True).wait_send()
    put_flag.wait()


def solution(mesh):
    nlat, nlon = mesh.shape["lat"], mesh.shape["lon"]

    def body(tracers, offsets, target, band_mask):
        nt = tracers.shape[0]
        nb = nlon // ZGROUP
        vmem, dma = pltpu.VMEM, pltpu.SemaphoreType.DMA
        operands = tuple(pltpu.with_memory_space_constraint(a, pltpu.HBM) for a in (
            tracers.reshape(nt, 32, 128),
            offsets.reshape(64, 128),
            jnp.transpose(target, (1, 2, 0)).reshape(32, nt),
            band_mask,
        ))

        def run(dense):
            return pl.pallas_call(
                functools.partial(kernel, dense, nt, nlat, nlon),
                out_shape=[
                    jax.ShapeDtypeStruct((TP * 32, 128), F32),
                    jax.ShapeDtypeStruct((1,), jnp.int32),
                ],
                in_specs=[pl.BlockSpec(memory_space=pltpu.HBM)] * 4,
                out_specs=[pl.BlockSpec(memory_space=pltpu.VMEM), pl.BlockSpec(memory_space=pltpu.HBM)],
                scratch_shapes=[
                    vmem((TP * PITCH, 128), F32),
                    vmem((2 * BANDS * TP, KW), BF16),
                    vmem((72, 128), jnp.int32),
                    vmem((32, nt), F32),
                    pltpu.SMEM((16,), jnp.int32),
                    vmem((2, TP, 128), F32),
                    vmem((2, TP, 128), F32),
                    vmem((40, 128), jnp.int32),
                    vmem((2, 8, TP, 128), F32),
                    vmem((2, 8, TP, 128), F32),
                    vmem((32, TP, 128), F32),
                    vmem((2 * KW, 128), BF16),
                    vmem((KW, 256), BF16),
                    vmem((128, 128), F32),
                    pltpu.SMEM((1,), jnp.int32),
                    vmem((2, ZGROUP, 16, 128), F32),
                    vmem((2, nb, 16, 128), F32),
                    vmem((2, 16, 128), jnp.int32),
                    vmem((2, 16, SLOTS), jnp.int32),
                    vmem((1024, SLOTS), BF16),
                    vmem((2, SLOTS, 1024), BF16),
                    vmem((2, 1, 128), F32),
                    vmem((nlat // 2, 1, 128), F32),
                    dma((4,)), dma((2,)), dma((2,)), dma((2,)), dma((2,)), dma((2, 8)), dma((2, 8)),
                    dma((2, ZGROUP)), dma((2, ZGROUP)), dma((2, nb)), dma((2, nb)), dma((nlat // 2,)), dma((nlat // 2,)),
                ],
                compiler_params=pltpu.CompilerParams(
                    collective_id=int(dense), has_side_effects=True, vmem_limit_bytes=50000000
                ),
            )(*operands)

        out, flag = run(False)
        out = lax.cond(flag[0] > 0, lambda: run(True)[0], lambda: out)
        return out[0:nt * 32].reshape(tracers.shape)

    placed = (
        P(None, None, "lat", "lon"),
        P(None, None, "lat", "lon"),
        P(None, None, "lat"),
        P("lat"),
    )
    return jax.shard_map(
        body, mesh=mesh, in_specs=placed, out_specs=P(None, None, "lat", "lon"), check_vma=False
    )
```
